256 devices in a mesh: tok: 128 (over x, z, y), exp: 2 (over core).
Axes of the slice: x: 4, y: 4, z: 8, core: 2. Of those that a mesh axis runs over, the one named last changes fastest.
Arguments:
- activations: bfloat16 [3072, 14336], P(('tok', 'exp')), may hold values from -6 to 6
- expert_ids: int32 [3072, 2], P(('tok', 'exp')), may hold values from 0 to 7, all different within a row; in each aligned block of 12 rows (0 to 11, 12 to 23, ...) at most 4 rows name the same one
Outputs:
- hessian: float32 [2, 14336, 14336], P('exp', 'tok')
The draws below stay inside these ranges and needn't reach their ends.
Inputs may be any that keep to these rules, and one draw needn't show every extreme that they name: `expert_ids`: each row names 2 different experts. Among the 12 rows of one device no expert is named more than 4 times, some expert exactly 4 times; every expert is named by some row.
All inputs are finite; a program needn't handle non-finite values.
Results may differ from the reference program's by a relative error of at most 0.0003.
Values may be sent and summed in bfloat16 or wider, within the bound.
A program may use at most 128 MiB of HBM per device.

```python
import math
import jax
import jax.numpy as jnp
import numpy as np
from jax import lax

FF = 14336
NUM_EXPERTS = 8
TOP = 2
TOK_DEV = 12
CAP = 4
EXPERTS = 2
TOKENS = 3072


def block_scale(stream_key, dims, shards, low, high):
    loudness, own = 1.0, jax.random.fold_in(stream_key, 6)
    for dim, shards_of in shards:
        steps = jnp.exp(jax.random.uniform(jax.random.fold_in(own, dim), (shards_of,), jnp.float32, low / len(shards), high / len(shards)))
        loudness = loudness * jnp.repeat(steps, dims[dim] // shards_of).reshape([-1 if axis == dim else 1 for axis in range(len(dims))])
    return loudness


def routed_block(key, own, number, rows, count, top, limit, slope):
    sequence = jax.random.permutation(key, count)
    heavy_load, common = shares(count, rows * top, limit, slope, True), shares(count, rows * top, limit, slope, False)
    places = jnp.arange(count)

    def named(lengths, rotation):
        used = int((lengths > 0).sum())
        fixed = max(1, used // 4)
        passed = fixed + (places - fixed + rotation * (used - fixed)) % max(1, count - fixed)
        return jnp.zeros((count,), jnp.int32).at[sequence[jnp.where(places < fixed, places, passed)]].set(jnp.asarray(lengths, jnp.int32))

    lengths = jnp.where(number % 4 == 0, named(heavy_load, number // 4), named(common, number - number // 4 - 1))
    mixed = jax.random.permutation(jax.random.fold_in(own, 3), count)
    donor, receiver = mixed[0:count // 2 * 2:2], mixed[1:count // 2 * 2:2]
    slack = jnp.minimum(lengths[donor] - 1, limit - lengths[receiver]) // 2
    slack = jnp.where((donor == sequence[0]) | (receiver == sequence[0]) | (lengths[receiver] == 0), 0, jnp.maximum(slack, 0))
    passed = jax.random.randint(jax.random.fold_in(own, 4), (count // 2,), 0, 1 << 20) % (slack + 1)
    lengths = lengths.at[donor].add(-passed).at[receiver].add(passed)
    labels = jnp.searchsorted(jnp.cumsum(lengths), jnp.arange(rows * top), side="right").astype(jnp.int32)
    table = labels.reshape(top, rows).T
    table = table[jax.random.permutation(jax.random.fold_in(own, 1), rows)]
    rotation = jax.random.randint(jax.random.fold_in(own, 2), (rows, 1), 0, top)
    return jnp.take_along_axis(table, (jnp.arange(top)[None, :] + rotation) % top, axis=1)


def shares(count, total, bound, lean, full):
    weights = [(1 << 20) // math.isqrt(grade ** lean) + 1 for grade in range(1, count + 1)]
    largest = bound if full else min(bound, max(-(-total // count), total * weights[0] // sum(weights)))
    least = 1 if total - largest >= count - 1 else 0
    given, rest = [largest] + [least] * (count - 1), total - largest - least * (count - 1)
    while rest > 0:
        movable = [i for i in range(1, count) if given[i] < largest] or [i for i in range(1, count) if given[i] < bound]
        pool, budget = sum([weights[i] for i in movable]), rest
        for i in movable:
            addition = min(bound - given[i], max(1, budget * weights[i] // pool), rest)
            given[i] = given[i] + addition
            rest = rest - addition
    return np.array(given)


def normal_values(rng, dims, spread, most, shards=(), held_as=jnp.bfloat16):
    drawn = spread * jax.random.normal(rng, dims, jnp.float32)
    if shards:
        drawn = drawn * block_scale(rng, dims, shards, -0.22, 0.18)
    return jnp.clip(drawn, -most, most).astype(held_as)


def setup_inputs(seed: int = 0) -> dict:
    splits = jax.random.split(jax.random.key(seed), 3)
    activations = normal_values(splits[0], (TOKENS, FF), 1.0, 6.0, ((0, 256),))
    expert_ids_keys = jax.random.split(jax.random.fold_in(splits[1], 1), TOKENS // TOK_DEV)
    expert_ids_turns = jax.random.permutation(jax.random.fold_in(splits[1], 3), TOKENS // TOK_DEV)
    expert_ids = jax.vmap(lambda own, number: routed_block(jax.random.fold_in(splits[1], 2), own, number, TOK_DEV, NUM_EXPERTS, TOP, CAP, 2))(expert_ids_keys, expert_ids_turns).reshape((TOKENS, TOP))
    return dict(activations=activations, expert_ids=expert_ids)


def reference(activations, expert_ids):
    features = activations.astype(jnp.float32)

    def one_expert(expert):
        routed = jnp.any(expert_ids == expert, axis=1).astype(jnp.float32)
        count = jnp.sum(routed)
        masked = features * routed[:, None]
        gram = jnp.dot(masked.T, features, precision=lax.Precision.HIGHEST, preferred_element_type=jnp.float32)
        return gram * (2.0 / count)

    return lax.map(one_expert, jnp.arange(EXPERTS, dtype=jnp.int32))
```

```python
import jax
import jax.numpy as jnp
from jax import lax
from jax.sharding import Mesh
from jax.sharding import PartitionSpec as P

CAP = 4
LANES = 128
RING = "tok_2"
PLANE = ("tok_0", "tok_1")
TOK = ("tok_0", "tok_1", "tok_2")
TOK_EXP = ("tok_0", "tok_1", "tok_2", "exp")


def place_tokens(activations, expert_ids, window_size):
    expert_labels = jnp.arange(window_size, dtype=jnp.int32)
    routed = jnp.any(expert_ids[:, :, None] == expert_labels[None, None, :], axis=1).astype(
        jnp.int32
    )
    ranking = jnp.cumsum(routed, axis=0) - 1
    slot_labels = jnp.arange(CAP, dtype=jnp.int32)
    placement = (routed.T[:, None, :] == 1) & (ranking.T[:, None, :] == slot_labels[None, :, None])
    placement_b = placement.astype(jnp.bfloat16)
    send_slots = jnp.einsum(
        "gct,tf->gcf", placement_b, activations, preferred_element_type=jnp.float32
    ).astype(jnp.bfloat16)
    return send_slots, jnp.sum(routed, axis=0)


def shards(activations, expert_ids):
    experts = lax.axis_size("exp")
    ring = lax.axis_size(RING)
    ff = activations.shape[1]
    tiles = ff // (ring * LANES)
    slots, counts = place_tokens(activations, expert_ids, experts)
    slots = slots.reshape(experts, CAP, tiles, ring, LANES).transpose(3, 0, 1, 2, 4)
    slots = slots.reshape(ring * experts, CAP, tiles * LANES)
    own = lax.all_to_all(slots, (RING, "exp"), split_axis=0, concat_axis=0, tiled=True)
    own = own.reshape(ring * experts * CAP, tiles * LANES)
    total = counts.astype(jnp.float32)
    for axis in TOK_EXP:
        total = lax.psum(total, axis)
    routed_total = total[lax.axis_index("exp")]

    cols = lax.all_gather(own, PLANE, axis=0, tiled=True)
    group = lax.axis_index("tok_0") * lax.axis_size("tok_1") + lax.axis_index("tok_1")
    rows = ff // lax.axis_size(PLANE)
    first = (group * rows) // LANES
    y = lax.axis_index(RING)
    mine = (first - y + ring - 1) // ring
    left = lax.dynamic_slice_in_dim(cols, mine * LANES, LANES, axis=1)
    left = lax.all_gather(left, RING, axis=0)
    order = (first + jnp.arange(ring)) % ring
    left = jnp.take(left, order, axis=0).transpose(1, 0, 2).reshape(cols.shape[0], ring * LANES)
    left = lax.dynamic_slice_in_dim(left, group * rows - first * LANES, rows, axis=1)
    product = lax.dot_general(
        left, cols, (((0,), (0,)), ((), ())), preferred_element_type=jnp.float32
    )
    out = lax.all_to_all(
        product.reshape(ring, rows // ring, tiles * LANES), RING, split_axis=0, concat_axis=0, tiled=True
    )
    out = out * (2.0 / routed_total)
    out = out.reshape(ring, rows // ring, tiles, LANES).transpose(1, 2, 0, 3)
    return out.reshape(1, rows // ring, ff)


def solution(mesh):
    split = Mesh(
        mesh.devices.reshape(4, 8, 4, mesh.shape["exp"]), ("tok_0", "tok_1", "tok_2", "exp")
    )
    return jax.shard_map(
        shards,
        mesh=split,
        in_specs=(P(TOK_EXP, None), P(TOK_EXP, None)),
        out_specs=P("exp", TOK, None),
        check_vma=False,
    )
```

```python
import functools

import jax
import jax.numpy as jnp
from jax import lax
from jax.experimental import pallas as pl
from jax.experimental.pallas import tpu as pltpu
from jax.sharding import Mesh
from jax.sharding import PartitionSpec as P

CAP = 4
LANES = 128
AX, AZ, AY, AE = "tok_0", "tok_1", "tok_2", "exp"
TOK = (AX, AZ, AY)
TOK_EXP = (AX, AZ, AY, AE)
NX, NZ, NY, NE = 4, 8, 4, 2
TOP_CODE = 32767.0

CHUNKS = ((1, 2), (2, 3), (2, 3), (2, 3), (2, 3), (1, 2), (1, 1))
FIRST = (0, 0, 1, 1, 2, 2, 3)
SECOND_Z = (2, 3, 4, 5, 6, 7, 8)
SECOND_X = (4, 5, 6, 7, 8, 9, 10)


def place_tokens(activations, expert_ids, window_size):
    expert_labels = jnp.arange(window_size, dtype=jnp.int32)
    routed = jnp.any(expert_ids[:, :, None] == expert_labels[None, None, :], axis=1).astype(
        jnp.int32
    )
    ranking = jnp.cumsum(routed, axis=0) - 1
    slot_labels = jnp.arange(CAP, dtype=jnp.int32)
    placement = (routed.T[:, None, :] == 1) & (ranking.T[:, None, :] == slot_labels[None, :, None])
    placement_b = placement.astype(jnp.bfloat16)
    send_slots = jnp.einsum(
        "gct,tf->gcf", placement_b, activations, preferred_element_type=jnp.float32
    ).astype(jnp.bfloat16)
    marks = jnp.sum(placement.astype(jnp.float32), axis=2).astype(jnp.bfloat16)
    return send_slots, marks


def remote(src, dst, send, recv, **where):
    return pltpu.make_async_remote_copy(
        src_ref=src,
        dst_ref=dst,
        send_sem=send,
        recv_sem=recv,
        device_id=where,
        device_id_type=pl.DeviceIdType.MESH,
    )


def wrap(index, count):
    return lax.rem(index + count, count)


class Ring:
    def __init__(self, axis, count, view, extent, send, recv):
        self.axis, self.count, self.view, self.extent = axis, count, view, extent
        self.send, self.recv = send, recv
        self.me = lax.axis_index(axis)
        self.steps = count // 2

    def copy(self, step, way):
        sign = 1 if way == 0 else -1
        block = wrap(self.me - sign * (step - 1), self.count)
        half = self.extent // 2
        at, size = (way * half, half) if step == self.steps else (0, self.extent)
        ref = self.view(block, at, size)
        to = wrap(self.me + sign, self.count)
        return remote(ref, ref, self.send.at[way], self.recv.at[step - 1, way], **{self.axis: to})

    def run(self, step):
        for way in (0, 1):
            now = self.copy(step, way)
            if step > 1:
                before = self.copy(step - 1, way)
                before.wait_recv()
                before.wait_send()
            now.start()

    def finish(self):
        for way in (0, 1):
            self.copy(self.steps, way).wait()


def kernel(
    slots, codes, scales,
    arrived, own, left1, left4, left, gx, gz, prod, code, scale, cx, cz,
    s_y, r_y, s_c, r_c, s_l1, r_l1, s_l2, r_l2, s_l3, r_l3,
    s_xf, r_xf, s_zs, r_zs, s_zf, r_zf, s_xs, r_xs, s_o, r_o, l_o,
):
    x, z, y, e = (lax.axis_index(a) for a in (AX, AZ, AY, AE))
    rows = prod.shape[0] // NY
    slab = NY * NE * CAP
    marks_at = own.shape[1]

    pairs = [(dy, de) for dy in range(NY) for de in range(NE) if (dy, de) != (0, 0)]
    barrier = pltpu.get_barrier_semaphore()
    for d in range(1, NX):
        pl.semaphore_signal(barrier, inc=1, device_id={AX: wrap(x + d, NX)}, device_id_type=pl.DeviceIdType.MESH)
    for d in range(1, NZ):
        pl.semaphore_signal(barrier, inc=1, device_id={AZ: wrap(z + d, NZ)}, device_id_type=pl.DeviceIdType.MESH)
    for dy, de in pairs:
        pl.semaphore_signal(barrier, inc=1, device_id={AY: wrap(y + dy, NY), AE: wrap(e + de, NE)}, device_id_type=pl.DeviceIdType.MESH)
    pl.semaphore_wait(barrier, NX - 1 + NZ - 1 + len(pairs))

    me = y * NE + e
    fetch = []
    for i, (dy, de) in enumerate(pairs):
        ty, te = wrap(y + dy, NY), wrap(e + de, NE)
        c = remote(slots.at[ty * NE + te], arrived.at[me], s_y.at[i], r_y.at[i], **{AY: ty, AE: te})
        c.start()
        fetch.append(c)
    arrived[me] = slots[me]
    for c in fetch:
        c.wait()

    mine = jnp.concatenate(
        [arrived[i, :, :marks_at].astype(jnp.float32) for i in range(NY * NE)], axis=0
    ).astype(jnp.bfloat16)
    own[...] = mine
    at_x = pl.ds(pl.multiple_of(x * slab, slab), slab)
    tile = 0
    spans = []
    px = pz = 0
    for a, b in CHUNKS:
        gx[z, at_x, px * LANES:(px + a) * LANES] = own[:, tile * LANES:(tile + a) * LANES]
        gz[z, at_x, pz * LANES:(pz + b) * LANES] = own[:, (tile + a) * LANES:(tile + a + b) * LANES]
        spans.append((tile, a, b, px, pz))
        tile, px, pz = tile + a + b, px + a, pz + b
    left1[at_x, :] = own[:, pl.ds(pl.multiple_of(x * left1.shape[1], LANES), left1.shape[1])]
    marks = sum(
        jnp.sum(arrived[i, :, marks_at:].astype(jnp.float32), axis=0, keepdims=True)
        for i in range(NY * NE)
    )
    cx[x] = jnp.broadcast_to(marks, cx.shape[1:])

    def rows_of(block, at, size):
        return pl.ds(pl.multiple_of(block * slab + at, 8), size)

    rings = []
    for c, (_, a, b, px, pz) in enumerate(spans):
        on_x, on_z = pl.ds(px * LANES, a * LANES), pl.ds(pz * LANES, b * LANES)
        rings.append((
            Ring(AX, NX, lambda k, at, m, w=on_x: gx.at[z, rows_of(k, at, m), w], slab, s_xf.at[c], r_xf.at[c]),
            Ring(AZ, NZ, lambda k, at, m, w=on_x: gx.at[k, pl.ds(at, m), w], NX * slab, s_zs.at[c], r_zs.at[c]),
            Ring(AZ, NZ, lambda k, at, m, w=on_z: gz.at[k, rows_of(x, at, m), w], slab, s_zf.at[c], r_zf.at[c]),
            Ring(AX, NX, lambda k, at, m, w=on_z: gz.at[pl.ds(at, m), rows_of(k, 0, slab), w], NZ, s_xs.at[c], r_xs.at[c]),
        ))

    def left_step1():
        out = []
        for d in range(1, NX):
            to = wrap(x + d, NX)
            w = left1.shape[1]
            c = remote(
                own.at[:, pl.ds(pl.multiple_of(to * w, LANES), w)], left1.at[at_x, :],
                s_l1.at[d], r_l1.at[d], **{AX: to},
            )
            c.start()
            out.append(c)
            c = remote(cx.at[x], cx.at[x], s_c.at[d], r_c.at[d], **{AX: to})
            c.start()
            out.append(c)
        return out

    def local_tile(zz):
        return lax.div(lax.div(7 * zz, 2) - y + (NY - 1), NY)

    def left_step2():
        cz[z] = sum(cx[i] for i in range(NX))
        out = []
        for d in (1, 7, 2, 6, 3, 5, 4):
            to = wrap(z + d, NZ)
            c = remote(
                left1.at[:, pl.ds(pl.multiple_of(local_tile(to) * LANES, LANES), LANES)], left4.at[y, z],
                s_l2.at[d], r_l2.at[d], **{AZ: to},
            )
            c.start()
            n = remote(cz.at[z], cz.at[z], s_c.at[NX + d], r_c.at[NX + d], **{AZ: to})
            n.start()
            out.append((c, n))
        left4[y, z] = left1[:, pl.ds(pl.multiple_of(local_tile(z) * LANES, LANES), LANES)]
        return out

    def left_step3(d):
        piece = wrap(z - d, NZ)
        out = []
        for dy in range(1, NY):
            c = remote(left4.at[y, piece], left4.at[y, piece], s_l3.at[d, dy], r_l3.at[d, dy], **{AY: wrap(y + dy, NY)})
            c.start()
            out.append(c)
        return out

    low = lax.div(7 * z, 2)
    off = pl.multiple_of(lax.rem(z, 2) * (LANES // 2), LANES // 2)
    k_all = NZ * NX * slab

    def transpose_left():
        for p in range(NY):
            yp = lax.rem(low + p, NY)
            for s in range(NZ):
                left[p * LANES:(p + 1) * LANES, s * LANES:(s + 1) * LANES] = left4[yp, s].T

    ways_out = []

    def multiply(c):
        t, a, b, px, pz = spans[c]
        w = (a + b) * LANES
        right = jnp.concatenate(
            [gx[:, :, px * LANES:(px + a) * LANES].reshape(k_all, a * LANES),
             gz[:, :, pz * LANES:(pz + b) * LANES].reshape(k_all, b * LANES)], axis=1)
        prod[:, :w] = jnp.dot(left[pl.ds(off, NY * rows), :], right, preferred_element_type=jnp.float32)
        at = pl.ds(t * LANES, w)
        factor = 2.0 / jnp.sum(cz[:, 0:1, 0:1], axis=0)

        def encode(i, carry):
            d = lax.rem(i + 1, NY)
            to = lax.rem(y + d, NY)
            v = prod[pl.ds(pl.multiple_of(to * rows, 16), rows), :w]
            m = jnp.max(jnp.abs(v), axis=0, keepdims=True)
            r = jnp.where(m > 0.0, 1.0 / jnp.where(m > 0.0, m, 1.0), 0.0)
            u = (jnp.sqrt(jnp.abs(v) * r) * TOP_CODE + 0.5).astype(jnp.int32)
            code[to, :, at] = jnp.where(v < 0.0, -u, u).astype(jnp.int16)
            scale[to, :, at] = m * factor
            return carry

        lax.fori_loop(0, NY, encode, 0)
        for dy in (1, 3, 2):
            to = wrap(y + dy, NY)
            for k, (src, dst) in enumerate(((code, codes), (scale, scales))):
                cp = remote(src.at[to, :, at], dst.at[y, :, at], s_o.at[c, dy, k], r_o.at[c, dy, k], **{AY: to})
                cp.start()
                ways_out.append(cp)
        for k, (src, dst) in enumerate(((code, codes), (scale, scales))):
            cp = pltpu.make_async_copy(src.at[y, :, at], dst.at[y, :, at], l_o.at[c, k])
            cp.start()
            ways_out.append(cp)

    n = len(CHUNKS)
    last = max(SECOND_Z[-1] + NZ // 2, SECOND_X[-1] + NX // 2)
    done1 = done2 = None
    done3 = []
    ready = False
    for r in range(last + 1):
        for c in range(n):
            xf, zs, zf, xs = rings[c]
            for ring, start in ((zs, SECOND_Z[c]), (xs, SECOND_X[c]), (zf, FIRST[c]), (xf, FIRST[c])):
                step = r - start + 1
                if 1 <= step <= ring.steps:
                    if ring is zs and step == 1:
                        xf.finish()
                    if ring is xs and step == 1:
                        zf.finish()
                    ring.run(step)
                elif step == ring.steps + 1 and ring in (zs, xs):
                    ring.finish()
            if r == 0 and c == 0:
                done1 = left_step1()
        if r == 1:
            for cp in done1:
                cp.wait()
            done2 = left_step2()
            done3 += left_step3(0)
        if r in (2, 3):
            for i, d in enumerate((1, 7, 2, 6, 3, 5, 4)):
                if (r == 2) == (i < 4):
                    for cp in done2[i]:
                        cp.wait()
                    done3 += left_step3(d)
        for c in range(n):
            if r == max(SECOND_Z[c] + NZ // 2, SECOND_X[c] + NX // 2):
                if not ready:
                    for cp in done3:
                        cp.wait()
                    transpose_left()
                    ready = True
                multiply(c)
    for cp in ways_out:
        cp.wait()


def exchange(slots):
    n = len(CHUNKS)
    tiles = sum(a + b for a, b in CHUNKS)
    t_x, t_z = (sum(c[i] for c in CHUNKS) for i in (0, 1))
    slab = NY * NE * CAP
    wide = max(a + b for a, b in CHUNKS) * LANES
    rows = tiles * LANES // (NX * NZ)
    bf16, f32, i16 = jnp.bfloat16, jnp.float32, jnp.int16
    dma = pltpu.SemaphoreType.DMA
    hbm = pl.BlockSpec(memory_space=pltpu.HBM)
    return pl.pallas_call(
        kernel,
        out_shape=(
            jax.ShapeDtypeStruct((NY, rows, tiles * LANES), i16),
            jax.ShapeDtypeStruct((NY, 1, tiles * LANES), f32),
        ),
        in_specs=[pl.BlockSpec(memory_space=pltpu.VMEM)],
        out_specs=(hbm, hbm),
        scratch_shapes=[
            pltpu.VMEM((NY * NE, CAP, (tiles + 1) * LANES), bf16),
            pltpu.VMEM((slab, tiles * LANES), bf16),
            pltpu.VMEM((NX * slab, tiles * LANES // NX), bf16),
            pltpu.VMEM((NY, NZ, NX * slab, LANES), bf16),
            pltpu.VMEM((NY * LANES, NZ * NX * slab), bf16),
            pltpu.VMEM((NZ, NX * slab, t_x * LANES), bf16),
            pltpu.VMEM((NZ, NX * slab, t_z * LANES), bf16),
            pltpu.VMEM((NY * rows, wide), f32),
            pltpu.VMEM((NY, rows, tiles * LANES), i16),
            pltpu.VMEM((NY, 1, tiles * LANES), f32),
            pltpu.VMEM((NX, 8, LANES), f32),
            pltpu.VMEM((NZ, 8, LANES), f32),
            dma((NY * NE,)), dma((NY * NE,)),
            dma((NX + NZ,)), dma((NX + NZ,)),
            dma((NX,)), dma((NX,)),
            dma((NZ,)), dma((NZ,)),
            dma((NZ, NY)), dma((NZ, NY)),
            dma((n, 2)), dma((n, NX // 2, 2)),
            dma((n, 2)), dma((n, NZ // 2, 2)),
            dma((n, 2)), dma((n, NZ // 2, 2)),
            dma((n, 2)), dma((n, NX // 2, 2)),
            dma((n, NY, 2)), dma((n, NY, 2)), dma((n, 2)),
        ],
        compiler_params=pltpu.CompilerParams(
            collective_id=0, has_side_effects=True, vmem_limit_bytes=48 * 1024 * 1024
        ),
        name="exchange",
    )(slots)


def decode_kernel(codes, scales, out):
    for j in range(codes.shape[2] // LANES):
        at = slice(j * LANES, (j + 1) * LANES)
        for y in range(NY):
            u = codes[y, :, at].astype(jnp.int32).astype(jnp.float32) * (1.0 / TOP_CODE)
            to = (j * NY + y) * LANES
            out[0, :, to:to + LANES] = u * jnp.abs(u) * scales[y, :, at]


def decode(codes, scales):
    _, rows, width = codes.shape
    step = 4 * LANES
    return pl.pallas_call(
        decode_kernel,
        grid=(width // step,),
        in_specs=[
            pl.BlockSpec((NY, rows, step), lambda i: (0, 0, i)),
            pl.BlockSpec((NY, 1, step), lambda i: (0, 0, i)),
        ],
        out_specs=pl.BlockSpec((1, rows, step * NY), lambda i: (0, 0, i)),
        out_shape=jax.ShapeDtypeStruct((1, rows, width * NY), jnp.float32),
        name="decode",
    )(codes, scales)


def shards(activations, expert_ids):
    ff = activations.shape[1]
    tiles = ff // (NY * LANES)
    slots, marks = place_tokens(activations, expert_ids, NE)
    slots = slots.reshape(NE, CAP, tiles, NY, LANES).transpose(3, 0, 1, 2, 4)
    slots = slots.reshape(NY, NE, CAP, tiles * LANES)
    marks = jnp.broadcast_to(marks[None, :, :, None], (NY, NE, CAP, LANES))
    slots = jnp.concatenate([slots, marks], axis=3).reshape(NY * NE, CAP, (tiles + 1) * LANES)
    codes, scales = exchange(slots)
    return decode(codes, scales)


def solution(mesh):
    split = Mesh(mesh.devices.reshape(NX, NZ, NY, NE), TOK_EXP)
    return jax.shard_map(
        shards,
        mesh=split,
        in_specs=(P(TOK_EXP, None), P(TOK_EXP, None)),
        out_specs=P(AE, TOK, None),
        check_vma=False,
    )
```

```python
import functools

import jax
import jax.numpy as jnp
from jax import lax
from jax.experimental import pallas as pl
from jax.experimental.pallas import tpu as pltpu
from jax.sharding import Mesh
from jax.sharding import PartitionSpec as P

CAP = 4
LANES = 128
AX, AZ, AY, AE = "tok_0", "tok_1", "tok_2", "exp"
TOK = (AX, AZ, AY)
TOK_EXP = (AX, AZ, AY, AE)
NX, NZ, NY, NE = 4, 8, 4, 2
TOP_CODE = 32767.0

CHUNKS = ((1, 1), (1, 2), (1, 4), (1, 1), (1, 3), (2, 2), (1, 2), (2, 3))
DIRECT = 1
ORDER = (
    ("qz", 1, 1), ("qz", 6, 1), ("qz", 2, 1), ("l1", 0, 1), ("px", 1, 1), ("px", 0, 1), ("px", 2, 1), ("px", 3, 1),
    ("px", 6, 1), ("px", 5, 1), ("px", 4, 1), ("px", 7, 1), ("qz", 0, 1), ("qz", 3, 1), ("qz", 7, 1), ("qz", 1, 2),
    ("qz", 6, 2), ("qz", 4, 1), ("qz", 2, 2), ("qz", 5, 1), ("qz", 3, 2), ("l2", 0, 4), ("l3", 0, 0), ("qz", 1, 3),
    ("l2", 0, 3), ("qx", 0, 1), ("qz", 2, 3), ("pz", 0, 1), ("qz", 1, 4), ("qz", 5, 2), ("qx", 0, 2), ("qz", 3, 3),
    ("pz", 2, 1), ("l3", 0, 4), ("pz", 1, 1), ("l2", 0, 1), ("qz", 2, 4), ("l3", 0, 3), ("pz", 0, 2), ("qx", 1, 1),
    ("qz", 4, 2), ("l2", 0, 2), ("pz", 1, 2), ("l3", 0, 1), ("qx", 2, 1), ("qz", 3, 4), ("pz", 2, 2), ("pz", 0, 3),
    ("pz", 3, 1), ("qx", 1, 2), ("pz", 6, 1), ("qz", 4, 3), ("l3", 0, 2), ("qx", 3, 1), ("pz", 1, 3), ("pz", 2, 3),
    ("pz", 0, 4), ("pz", 4, 1), ("pz", 5, 1), ("qz", 4, 4), ("pz", 1, 4), ("qx", 2, 2), ("pz", 2, 4), ("qz", 5, 3),
    ("pz", 3, 2), ("mm", 0, 1), ("pz", 4, 2), ("qz", 7, 2), ("qx", 3, 2), ("qx", 4, 1), ("qz", 6, 3), ("mm", 1, 1),
    ("qz", 5, 4), ("pz", 3, 3), ("pz", 5, 2), ("mm", 2, 1), ("qz", 7, 3), ("qz", 6, 4), ("pz", 4, 3), ("qx", 5, 1),
    ("pz", 3, 4), ("pz", 7, 1), ("pz", 5, 3), ("qx", 4, 2), ("qx", 6, 1), ("pz", 4, 4), ("mm", 3, 1), ("qz", 7, 4),
    ("pz", 6, 2), ("qx", 5, 2), ("pz", 7, 2), ("pz", 5, 4), ("mm", 4, 1), ("qx", 7, 1), ("pz", 6, 3), ("pz", 7, 3),
    ("qx", 6, 2), ("mm", 5, 1), ("pz", 6, 4), ("pz", 7, 4), ("qx", 7, 2), ("mm", 6, 1), ("mm", 7, 1),
)


def place_tokens(activations, expert_ids, window_size):
    expert_labels = jnp.arange(window_size, dtype=jnp.int32)
    routed = jnp.any(expert_ids[:, :, None] == expert_labels[None, None, :], axis=1).astype(
        jnp.int32
    )
    ranking = jnp.cumsum(routed, axis=0) - 1
    slot_labels = jnp.arange(CAP, dtype=jnp.int32)
    placement = (routed.T[:, None, :] == 1) & (ranking.T[:, None, :] == slot_labels[None, :, None])
    placement_b = placement.astype(jnp.bfloat16)
    send_slots = jnp.einsum(
        "gct,tf->gcf", placement_b, activations, preferred_element_type=jnp.float32
    ).astype(jnp.bfloat16)
    marks = jnp.sum(placement.astype(jnp.float32), axis=2).astype(jnp.bfloat16)
    return send_slots, marks


def remote(src, dst, send, recv, **where):
    return pltpu.make_async_remote_copy(
        src_ref=src,
        dst_ref=dst,
        send_sem=send,
        recv_sem=recv,
        device_id=where,
        device_id_type=pl.DeviceIdType.MESH,
    )


def wrap(index, count):
    return lax.rem(index + count, count)


class Ring:
    def __init__(self, axis, count, view, extent, send, recv):
        self.axis, self.count, self.view, self.extent = axis, count, view, extent
        self.send, self.recv = send, recv
        self.me = lax.axis_index(axis)
        self.steps = count // 2

    def copy(self, step, way):
        sign = 1 if way == 0 else -1
        block = wrap(self.me - sign * (step - 1), self.count)
        half = self.extent // 2
        at, size = (way * half, half) if step == self.steps else (0, self.extent)
        ref = self.view(block, at, size)
        to = wrap(self.me + sign, self.count)
        return remote(ref, ref, self.send.at[way], self.recv.at[step - 1, way], **{self.axis: to})

    def run(self, step):
        for way in (0, 1):
            now = self.copy(step, way)
            if step > 1:
                before = self.copy(step - 1, way)
                before.wait_recv()
                before.wait_send()
            now.start()

    def finish(self):
        for way in (0, 1):
            self.copy(self.steps, way).wait()


class Direct:
    def __init__(self, axis, count, view, extent, send, recv, others):
        self.axis, self.count, self.view, self.extent = axis, count, view, extent
        self.send, self.recv, self.others = send, recv, others
        self.me = lax.axis_index(axis)
        self.steps = 1

    def run(self, step):
        ref = self.view(self.me, 0, self.extent)
        for d in sorted(range(1, self.count), key=lambda d: min(d, self.count - d)):
            to = wrap(self.me + d, self.count)
            remote(ref, ref, self.send, self.recv, **{self.axis: to}).start()

    def finish(self):
        remote(self.others, self.others, self.send, self.recv, **{self.axis: wrap(self.me + 1, self.count)}).wait()


def kernel(
    slots, codes, scales,
    arrived, own, left1, left4, left, gx, gz, prod, code, scale, cx, cz,
    s_y, r_y, s_c, r_c, s_l1, r_l1, s_l2, r_l2, s_l3, r_l3,
    s_xf, r_xf, s_zs, r_zs, s_zf, r_zf, s_xs, r_xs, s_zd, r_zd, s_o, r_o,
):
    x, z, y, e = (lax.axis_index(a) for a in (AX, AZ, AY, AE))
    rows = prod.shape[0] // NY
    slab = NY * NE * CAP
    marks_at = own.shape[1]

    pairs = [(dy, de) for dy in range(NY) for de in range(NE) if (dy, de) != (0, 0)]
    barrier = pltpu.get_barrier_semaphore()
    for d in range(1, NX):
        pl.semaphore_signal(barrier, inc=1, device_id={AX: wrap(x + d, NX)}, device_id_type=pl.DeviceIdType.MESH)
    for d in range(1, NZ):
        pl.semaphore_signal(barrier, inc=1, device_id={AZ: wrap(z + d, NZ)}, device_id_type=pl.DeviceIdType.MESH)
    for dy, de in pairs:
        pl.semaphore_signal(barrier, inc=1, device_id={AY: wrap(y + dy, NY), AE: wrap(e + de, NE)}, device_id_type=pl.DeviceIdType.MESH)
    pl.semaphore_wait(barrier, NX - 1 + NZ - 1 + len(pairs))

    me = y * NE + e
    for dy, de in pairs:
        ty, te = wrap(y + dy, NY), wrap(e + de, NE)
        remote(slots.at[ty * NE + te], arrived.at[me], s_y, r_y, **{AY: ty, AE: te}).start()
    arrived[me] = slots[me]
    most = pl.ds(0, len(pairs))
    remote(slots.at[most], arrived.at[most], s_y, r_y, **{AE: wrap(e + 1, NE)}).wait()

    mine = jnp.concatenate(
        [arrived[i, :, :marks_at].astype(jnp.float32) for i in range(NY * NE)], axis=0
    ).astype(jnp.bfloat16)
    own[...] = mine
    at_x = pl.ds(pl.multiple_of(x * slab, slab), slab)
    tile = 0
    spans = []
    px = pz = 0
    for a, b in CHUNKS:
        gx[z, at_x, px * LANES:(px + a) * LANES] = own[:, tile * LANES:(tile + a) * LANES]
        gz[z, at_x, pz * LANES:(pz + b) * LANES] = own[:, (tile + a) * LANES:(tile + a + b) * LANES]
        spans.append((tile, a, b, px, pz))
        tile, px, pz = tile + a + b, px + a, pz + b
    left1[at_x, :] = own[:, pl.ds(pl.multiple_of(x * left1.shape[1], LANES), left1.shape[1])]
    marks = sum(
        jnp.sum(arrived[i, :, marks_at:].astype(jnp.float32), axis=0, keepdims=True)
        for i in range(NY * NE)
    )
    cx[x] = jnp.broadcast_to(marks, cx.shape[1:])

    def rows_of(block, at, size):
        return pl.ds(pl.multiple_of(block * slab + at, 8), size)

    rings = []
    for c, (_, a, b, px, pz) in enumerate(spans):
        on_x, on_z = pl.ds(px * LANES, a * LANES), pl.ds(pz * LANES, b * LANES)
        rings.append((
            Direct(AX, NX, lambda k, at, m, w=on_x: gx.at[z, rows_of(k, at, m), w], slab, s_xf.at[c], r_xf.at[c],
                   gx.at[z, pl.ds(0, (NX - 1) * slab), on_x]),
            Ring(AZ, NZ, lambda k, at, m, w=on_x: gx.at[k, pl.ds(at, m), w], NX * slab, s_zs.at[c], r_zs.at[c]),
            Direct(AZ, NZ, lambda k, at, m, w=on_z: gz.at[k, rows_of(x, at, m), w], slab, s_zd.at[c], r_zd.at[c],
                   gz.at[pl.ds(0, NZ - 1), at_x, on_z])
            if c < DIRECT else
            Ring(AZ, NZ, lambda k, at, m, w=on_z: gz.at[k, rows_of(x, at, m), w], slab, s_zf.at[c], r_zf.at[c]),
            Ring(AX, NX, lambda k, at, m, w=on_z: gz.at[pl.ds(at, m), rows_of(k, 0, slab), w], NZ, s_xs.at[c], r_xs.at[c]),
        ))

    def left_step1():
        w = left1.shape[1]
        for d in range(1, NX):
            to = wrap(x + d, NX)
            remote(
                own.at[:, pl.ds(pl.multiple_of(to * w, LANES), w)], left1.at[at_x, :], s_l1, r_l1, **{AX: to}
            ).start()
            remote(cx.at[x], cx.at[x], s_c.at[0], r_c.at[0], **{AX: to}).start()

    def left_wait1():
        w, k = left1.shape[1], (NX - 1) * slab
        to = wrap(x + 1, NX)
        remote(own.at[:, pl.ds(0, (NX - 1) * w)], left1.at[pl.ds(0, k), :], s_l1, r_l1, **{AX: to}).wait()
        rest = cx.at[pl.ds(0, NX - 1)]
        remote(rest, rest, s_c.at[0], r_c.at[0], **{AX: to}).wait()
        cz[z] = sum(cx[i] for i in range(NX))
        left4[y, z] = left1[:, pl.ds(pl.multiple_of(local_tile(z) * LANES, LANES), LANES)]

    def local_tile(zz):
        return lax.div(lax.div(7 * zz, 2) - y + (NY - 1), NY)

    def left_copy2(d):
        to = wrap(z + d, NZ)
        return remote(
            left1.at[:, pl.ds(pl.multiple_of(local_tile(to) * LANES, LANES), LANES)], left4.at[y, z],
            s_l2.at[d], r_l2.at[d], **{AZ: to},
        )

    def left_step2(d):
        left_copy2(d).start()
        remote(cz.at[z], cz.at[z], s_c.at[1], r_c.at[1], **{AZ: wrap(z + d, NZ)}).start()

    def left_step3(d):
        piece = left4.at[y, wrap(z - d, NZ)]
        for dy in range(1, NY):
            remote(piece, piece, s_l3.at[dy], r_l3.at[dy], **{AY: wrap(y + dy, NY)}).start()

    def left_wait3():
        rest = cz.at[pl.ds(0, NZ - 1)]
        remote(rest, rest, s_c.at[1], r_c.at[1], **{AZ: wrap(z + 1, NZ)}).wait()
        for dy in range(1, NY):
            remote(left4.at[y], left4.at[wrap(y - dy, NY)], s_l3.at[dy], r_l3.at[dy], **{AY: wrap(y + dy, NY)}).wait()

    low = lax.div(7 * z, 2)
    off = pl.multiple_of(lax.rem(z, 2) * (LANES // 2), LANES // 2)
    k_all = NZ * NX * slab

    def transpose_left():
        for p in range(NY):
            yp = lax.rem(low + p, NY)
            for s in range(NZ):
                left[p * LANES:(p + 1) * LANES, s * LANES:(s + 1) * LANES] = left4[yp, s].T


    def multiply(c):
        t, a, b, px, pz = spans[c]
        w = (a + b) * LANES
        right = jnp.concatenate(
            [gx[:, :, px * LANES:(px + a) * LANES].reshape(k_all, a * LANES),
             gz[:, :, pz * LANES:(pz + b) * LANES].reshape(k_all, b * LANES)], axis=1)
        prod[:, :w] = jnp.dot(left[pl.ds(off, NY * rows), :], right, preferred_element_type=jnp.float32)
        factor = 2.0 / jnp.sum(cz[:, 0:1, 0:1], axis=0)

        def encode(i, carry):
            to = lax.rem(y + i + 1, NY)
            v = prod[pl.ds(pl.multiple_of(to * rows, 16), rows), :w]
            m = jnp.max(jnp.abs(v), axis=0, keepdims=True)
            r = jnp.where(m > 0.0, 1.0 / jnp.where(m > 0.0, m, 1.0), 0.0)
            u = (jnp.sqrt(jnp.abs(v) * r) * TOP_CODE + 0.5).astype(jnp.int32)
            code[to, :, t * LANES:t * LANES + w] = jnp.where(v < 0.0, -u, u).astype(jnp.int16)
            m = m * factor
            for j in range(a + b):
                scale[to, t + j] = m[:, j * LANES:(j + 1) * LANES]
            return carry

        lax.fori_loop(0, NY, encode, 0)
        for dy in (1, 3, 2):
            to = wrap(y + dy, NY)
            for j in range(t, t + a + b):
                remote(
                    code.at[to, :, pl.ds(j * LANES, LANES)], codes.at[:, lanes_of(j * NY + y)],
                    s_o.at[c, 0], r_o.at[c, 0], **{AY: to},
                ).start()
            remote(scale.at[to, pl.ds(t, a + b)], scales.at[pl.ds(t, a + b), y], s_o.at[c, 1], r_o.at[c, 1], **{AY: to}).start()
        for j in range(t, t + a + b):
            codes[:, lanes_of(j * NY + y)] = code[y, :, j * LANES:(j + 1) * LANES]
            scales[j, y] = scale[y, j]

    def lanes_of(tile):
        return pl.ds(pl.multiple_of(tile * LANES, LANES), LANES)

    def receive(c):
        k = (NY - 1) * (spans[c][1] + spans[c][2])
        to = wrap(y + 1, NY)
        whole = codes.at[:, pl.ds(0, k * LANES)]
        remote(whole, whole, s_o.at[c, 0], r_o.at[c, 0], **{AY: to}).wait()
        sizes = scales.at[pl.ds(0, k), 0]
        remote(sizes, sizes, s_o.at[c, 1], r_o.at[c, 1], **{AY: to}).wait()

    waited = False
    for kind, c, d in ORDER:
        if kind in ("l2", "l3") and not waited:
            left_wait1()
            waited = True
        if kind == "l1":
            left_step1()
        elif kind == "l2":
            for way in sorted({d, NZ - d}):
                left_step2(way)
        elif kind == "l3":
            for way in sorted({d, (NZ - d) % NZ}):
                if d:
                    left_copy2(way).wait()
                left_step3(way)
        elif kind == "mm":
            rings[c][1].finish()
            rings[c][3].finish()
            if c == 0:
                left_wait3()
                transpose_left()
            multiply(c)
        else:
            k = ("px", "pz", "qz", "qx").index(kind)
            if d == 1 and k in (1, 3):
                rings[c][k - 1].finish()
            rings[c][k].run(d)
    for c in range(len(CHUNKS)):
        receive(c)


def exchange(slots):
    n = len(CHUNKS)
    tiles = sum(a + b for a, b in CHUNKS)
    t_x, t_z = (sum(c[i] for c in CHUNKS) for i in (0, 1))
    slab = NY * NE * CAP
    wide = max(a + b for a, b in CHUNKS) * LANES
    rows = tiles * LANES // (NX * NZ)
    bf16, f32, i16 = jnp.bfloat16, jnp.float32, jnp.int16
    dma = pltpu.SemaphoreType.DMA
    vmem = pl.BlockSpec(memory_space=pltpu.VMEM)
    return pl.pallas_call(
        kernel,
        out_shape=(
            jax.ShapeDtypeStruct((rows, tiles * NY * LANES), i16),
            jax.ShapeDtypeStruct((tiles, NY, 1, LANES), f32),
        ),
        in_specs=[vmem],
        out_specs=(vmem, vmem),
        scratch_shapes=[
            pltpu.VMEM((NY * NE, CAP, (tiles + 1) * LANES), bf16),
            pltpu.VMEM((slab, tiles * LANES), bf16),
            pltpu.VMEM((NX * slab, tiles * LANES // NX), bf16),
            pltpu.VMEM((NY, NZ, NX * slab, LANES), bf16),
            pltpu.VMEM((NY * LANES, NZ * NX * slab), bf16),
            pltpu.VMEM((NZ, NX * slab, t_x * LANES), bf16),
            pltpu.VMEM((NZ, NX * slab, t_z * LANES), bf16),
            pltpu.VMEM((NY * rows, wide), f32),
            pltpu.VMEM((NY, rows, tiles * LANES), i16),
            pltpu.VMEM((NY, tiles, 1, LANES), f32),
            pltpu.VMEM((NX, 8, LANES), f32),
            pltpu.VMEM((NZ, 8, LANES), f32),
            dma(()), dma(()),
            dma((2,)), dma((2,)),
            dma(()), dma(()),
            dma((NZ,)), dma((NZ,)),
            dma((NY,)), dma((NY,)),
            dma((n,)), dma((n,)),
            dma((n, 2)), dma((n, NZ // 2, 2)),
            dma((n, 2)), dma((n, NZ // 2, 2)),
            dma((n, 2)), dma((n, NX // 2, 2)),
            dma((max(DIRECT, 1),)), dma((max(DIRECT, 1),)),
            dma((n, 2)), dma((n, 2)),
        ],
        compiler_params=pltpu.CompilerParams(
            collective_id=0, has_side_effects=True, vmem_limit_bytes=48 * 1024 * 1024
        ),
        name="exchange",
    )(slots)


def shards(activations, expert_ids):
    ff = activations.shape[1]
    tiles = ff // (NY * LANES)
    slots, marks = place_tokens(activations, expert_ids, NE)
    slots = slots.reshape(NE, CAP, tiles, NY, LANES).transpose(3, 0, 1, 2, 4)
    slots = slots.reshape(NY, NE, CAP, tiles * LANES)
    marks = jnp.broadcast_to(marks[None, :, :, None], (NY, NE, CAP, LANES))
    slots = jnp.concatenate([slots, marks], axis=3).reshape(NY * NE, CAP, (tiles + 1) * LANES)
    codes, scales = exchange(slots)
    u = codes.astype(jnp.float32) * (1.0 / TOP_CODE)
    return (u * jnp.abs(u) * scales.reshape(1, ff))[None]


def solution(mesh):
    split = Mesh(mesh.devices.reshape(NX, NZ, NY, NE), TOK_EXP)
    return jax.shard_map(
        shards,
        mesh=split,
        in_specs=(P(TOK_EXP, None), P(TOK_EXP, None)),
        out_specs=P(AE, TOK, None),
        check_vma=False,
    )
```

```python
import functools

import jax
import jax.numpy as jnp
from jax import lax
from jax.experimental import pallas as pl
from jax.experimental.pallas import tpu as pltpu
from jax.sharding import Mesh
from jax.sharding import PartitionSpec as P

CAP = 4
LANES = 128
AX, AZ, AY, AE = "tok_0", "tok_1", "tok_2", "exp"
TOK = (AX, AZ, AY)
TOK_EXP = (AX, AZ, AY, AE)
NX, NZ, NY, NE = 4, 8, 4, 2
TOP_CODE = 32767.0

CHUNKS = ((1, 1), (1, 3), (1, 2), (1, 3), (1, 1), (2, 3), (3, 1), (2, 2))
DIRECT = 1
ORDER = (
    ("l1", 0, 1), ("qz", 4, 1), ("px", 6, 1), ("qz", 7, 1), ("px", 7, 1), ("px", 5, 1), ("px", 0, 1), ("px", 4, 1),
    ("px", 2, 1), ("px", 3, 1), ("qz", 1, 1), ("px", 1, 1), ("qz", 2, 1), ("qz", 6, 1), ("qz", 0, 1), ("qz", 4, 2),
    ("qz", 7, 2), ("qz", 1, 2), ("qz", 6, 2), ("qz", 2, 2), ("qz", 5, 1), ("qz", 3, 1), ("l3", 0, 0), ("l2", 0, 1),
    ("qz", 4, 3), ("qz", 1, 3), ("qz", 6, 3), ("l2", 0, 2), ("qx", 0, 1), ("qz", 3, 2), ("l3", 0, 1), ("qz", 4, 4),
    ("pz", 0, 1), ("qz", 1, 4), ("qz", 2, 3), ("pz", 1, 1), ("l2", 0, 3), ("qx", 0, 2), ("qx", 4, 1), ("l3", 0, 2),
    ("qx", 1, 1), ("qz", 2, 4), ("pz", 0, 2), ("l2", 0, 4), ("pz", 1, 2), ("qx", 4, 2), ("qx", 2, 1), ("qz", 3, 3),
    ("pz", 0, 3), ("l3", 0, 3), ("pz", 2, 1), ("pz", 3, 1), ("pz", 1, 3), ("qz", 3, 4), ("qz", 5, 2), ("qx", 1, 2),
    ("l3", 0, 4), ("pz", 0, 4), ("pz", 2, 2), ("pz", 3, 2), ("pz", 1, 4), ("qx", 3, 1), ("pz", 5, 1), ("qx", 2, 2),
    ("qz", 5, 3), ("pz", 2, 3), ("mm", 0, 1), ("pz", 3, 3), ("mm", 0, 2), ("mm", 0, 3), ("pz", 4, 1), ("mm", 1, 1),
    ("pz", 5, 2), ("mm", 1, 2), ("mm", 1, 3), ("pz", 2, 4), ("qz", 5, 4), ("pz", 3, 4), ("qz", 6, 4), ("pz", 4, 2),
    ("qx", 3, 2), ("pz", 6, 1), ("mm", 2, 1), ("qx", 5, 1), ("qx", 6, 1), ("mm", 2, 2), ("pz", 5, 3), ("mm", 2, 3),
    ("pz", 4, 3), ("mm", 3, 1), ("pz", 6, 2), ("mm", 3, 2), ("mm", 3, 3), ("pz", 5, 4), ("pz", 4, 4), ("qz", 7, 3),
    ("pz", 7, 1), ("qx", 5, 2), ("pz", 6, 3), ("qx", 6, 2), ("mm", 4, 1), ("mm", 4, 2), ("mm", 4, 3), ("qz", 7, 4),
    ("pz", 7, 2), ("mm", 5, 1), ("mm", 5, 2), ("pz", 6, 4), ("qx", 7, 1), ("mm", 5, 3), ("pz", 7, 3), ("mm", 6, 1),
    ("mm", 6, 2), ("mm", 6, 3), ("qx", 7, 2), ("pz", 7, 4), ("mm", 7, 1), ("mm", 7, 2), ("mm", 7, 3),
)


def place_tokens(acts, ids, slots, chosen):
    named = ids[...]
    n = named.shape[0]
    row = lax.broadcasted_iota(jnp.int32, (n, n), 0)
    column = lax.broadcasted_iota(jnp.int32, (n, n), 1)
    slot = lax.broadcasted_iota(jnp.int32, (CAP, n), 0).astype(jnp.float32)
    picks = []
    for e in range(NE):
        routed = jnp.max(jnp.where(named == e, 1.0, 0.0), axis=1, keepdims=True)
        rank = jnp.sum(jnp.where(row < column, routed, 0.0), axis=0, keepdims=True)
        here = jnp.sum(jnp.where(row == column, routed, 0.0), axis=0, keepdims=True)
        picks.append(jnp.where((rank == slot) & (here > 0.0), 1.0, 0.0))
    width = slots.shape[2] - LANES
    pick = jnp.concatenate(picks, axis=0).astype(jnp.bfloat16)
    chosen[...] = jnp.dot(pick, acts[...], preferred_element_type=jnp.float32)
    for e in range(NE):
        mark = jnp.broadcast_to(jnp.sum(picks[e], axis=1, keepdims=True), (CAP, LANES)).astype(jnp.bfloat16)
        for y in range(NY):
            slots[y * NE + e, :, :width] = jnp.concatenate(
                [chosen[e * CAP:(e + 1) * CAP, (j * NY + y) * LANES:(j * NY + y + 1) * LANES] for j in range(width // LANES)],
                axis=1,
            ).astype(jnp.bfloat16)
            slots[y * NE + e, :, width:] = mark


def remote(src, dst, send, recv, **where):
    return pltpu.make_async_remote_copy(
        src_ref=src,
        dst_ref=dst,
        send_sem=send,
        recv_sem=recv,
        device_id=where,
        device_id_type=pl.DeviceIdType.MESH,
    )


def wrap(index, count):
    return lax.rem(index + count, count)


class Ring:
    def __init__(self, axis, count, view, extent, send, recv, two):
        self.axis, self.count, self.view, self.extent = axis, count, view, extent
        self.send, self.recv, self.two = send, recv, two
        self.me = lax.axis_index(axis)
        self.steps = count // 2

    def wait(self, step):
        ref = self.two if step < self.steps else self.view(self.me, 0, self.extent)
        to = wrap(self.me + 1, self.count)
        remote(ref, ref, self.send, self.recv.at[step - 1], **{self.axis: to}).wait()

    def run(self, step):
        if step > 1:
            self.wait(step - 1)
        half = self.extent // 2
        for way, sign in enumerate((1, -1)):
            at, size = (way * half, half) if step == self.steps else (0, self.extent)
            ref = self.view(wrap(self.me - sign * (step - 1), self.count), at, size)
            to = wrap(self.me + sign, self.count)
            remote(ref, ref, self.send, self.recv.at[step - 1], **{self.axis: to}).start()

    def finish(self):
        self.wait(self.steps)


class Direct:
    def __init__(self, axis, count, view, extent, send, recv, others):
        self.axis, self.count, self.view, self.extent = axis, count, view, extent
        self.send, self.recv, self.others = send, recv, others
        self.me = lax.axis_index(axis)
        self.steps = 1

    def run(self, step):
        ref = self.view(self.me, 0, self.extent)
        for d in sorted(range(1, self.count), key=lambda d: min(d, self.count - d)):
            to = wrap(self.me + d, self.count)
            remote(ref, ref, self.send, self.recv, **{self.axis: to}).start()

    def finish(self):
        remote(self.others, self.others, self.send, self.recv, **{self.axis: wrap(self.me + 1, self.count)}).wait()


def kernel(
    acts, ids, codes, scales,
    slots, chosen, arrived, own, left1, left4, left, gx, gz, prod, code, scale, cx, cz,
    s_y, r_y, s_c, r_c, s_l1, r_l1, s_l2, r_l2, s_l3, r_l3,
    s_xf, r_xf, s_zs, r_zs, s_zf, r_zf, s_xs, r_xs, s_zd, r_zd, s_o, r_o,
):
    x, z, y, e = (lax.axis_index(a) for a in (AX, AZ, AY, AE))
    rows = prod.shape[0] // NY
    slab = NY * NE * CAP
    marks_at = own.shape[1]

    pairs = [(dy, de) for dy in range(NY) for de in range(NE) if (dy, de) != (0, 0)]
    barrier = pltpu.get_barrier_semaphore()
    for d in range(1, NX):
        pl.semaphore_signal(barrier, inc=1, device_id={AX: wrap(x + d, NX)}, device_id_type=pl.DeviceIdType.MESH)
    for d in range(1, NZ):
        pl.semaphore_signal(barrier, inc=1, device_id={AZ: wrap(z + d, NZ)}, device_id_type=pl.DeviceIdType.MESH)
    for dy, de in pairs:
        pl.semaphore_signal(barrier, inc=1, device_id={AY: wrap(y + dy, NY), AE: wrap(e + de, NE)}, device_id_type=pl.DeviceIdType.MESH)
    place_tokens(acts, ids, slots, chosen)
    pl.semaphore_wait(barrier, NX - 1 + NZ - 1 + len(pairs))

    me = y * NE + e
    for dy, de in pairs:
        ty, te = wrap(y + dy, NY), wrap(e + de, NE)
        remote(slots.at[ty * NE + te], arrived.at[me], s_y, r_y, **{AY: ty, AE: te}).start()
    arrived[me] = slots[me]
    most = pl.ds(0, len(pairs))
    remote(slots.at[most], arrived.at[most], s_y, r_y, **{AE: wrap(e + 1, NE)}).wait()

    mine = jnp.concatenate(
        [arrived[i, :, :marks_at].astype(jnp.float32) for i in range(NY * NE)], axis=0
    ).astype(jnp.bfloat16)
    own[...] = mine
    at_x = pl.ds(pl.multiple_of(x * slab, slab), slab)
    tile = 0
    spans = []
    px = pz = 0
    for a, b in CHUNKS:
        gx[z, at_x, px * LANES:(px + a) * LANES] = own[:, tile * LANES:(tile + a) * LANES]
        gz[z, at_x, pz * LANES:(pz + b) * LANES] = own[:, (tile + a) * LANES:(tile + a + b) * LANES]
        spans.append((tile, a, b, px, pz))
        tile, px, pz = tile + a + b, px + a, pz + b
    left1[at_x, :] = own[:, pl.ds(pl.multiple_of(x * left1.shape[1], LANES), left1.shape[1])]
    marks = sum(
        jnp.sum(arrived[i, :, marks_at:].astype(jnp.float32), axis=0, keepdims=True)
        for i in range(NY * NE)
    )
    cx[x] = jnp.broadcast_to(marks, cx.shape[1:])

    def rows_of(block, at, size):
        return pl.ds(pl.multiple_of(block * slab + at, 8), size)

    rings = []
    for c, (_, a, b, px, pz) in enumerate(spans):
        on_x, on_z = pl.ds(px * LANES, a * LANES), pl.ds(pz * LANES, b * LANES)
        rings.append((
            Direct(AX, NX, lambda k, at, m, w=on_x: gx.at[z, rows_of(k, at, m), w], slab, s_xf.at[c], r_xf.at[c],
                   gx.at[z, pl.ds(0, (NX - 1) * slab), on_x]),
            Ring(AZ, NZ, lambda k, at, m, w=on_x: gx.at[k, pl.ds(at, m), w], NX * slab, s_zs.at[c], r_zs.at[c],
                 gx.at[pl.ds(0, 2), :, on_x]),
            Direct(AZ, NZ, lambda k, at, m, w=on_z: gz.at[k, rows_of(x, at, m), w], slab, s_zd.at[c], r_zd.at[c],
                   gz.at[pl.ds(0, NZ - 1), at_x, on_z])
            if c < DIRECT else
            Ring(AZ, NZ, lambda k, at, m, w=on_z: gz.at[k, rows_of(x, at, m), w], slab, s_zf.at[c], r_zf.at[c],
                 gz.at[pl.ds(0, 2), at_x, on_z]),
            Ring(AX, NX, lambda k, at, m, w=on_z: gz.at[pl.ds(at, m), rows_of(k, 0, slab), w], NZ, s_xs.at[c], r_xs.at[c],
                 gz.at[:, pl.ds(0, 2 * slab), on_z]),
        ))

    def left_step1():
        w = left1.shape[1]
        for d in range(1, NX):
            to = wrap(x + d, NX)
            remote(
                own.at[:, pl.ds(pl.multiple_of(to * w, LANES), w)], left1.at[at_x, :], s_l1, r_l1, **{AX: to}
            ).start()
            remote(cx.at[x], cx.at[x], s_c.at[0], r_c.at[0], **{AX: to}).start()

    def left_wait1():
        w, k = left1.shape[1], (NX - 1) * slab
        to = wrap(x + 1, NX)
        remote(own.at[:, pl.ds(0, (NX - 1) * w)], left1.at[pl.ds(0, k), :], s_l1, r_l1, **{AX: to}).wait()
        rest = cx.at[pl.ds(0, NX - 1)]
        remote(rest, rest, s_c.at[0], r_c.at[0], **{AX: to}).wait()
        cz[z] = sum(cx[i] for i in range(NX))
        left4[y, z] = left1[:, pl.ds(pl.multiple_of(local_tile(z) * LANES, LANES), LANES)]

    def local_tile(zz):
        return lax.div(lax.div(7 * zz, 2) - y + (NY - 1), NY)

    def left_copy2(d):
        to = wrap(z + d, NZ)
        return remote(
            left1.at[:, pl.ds(pl.multiple_of(local_tile(to) * LANES, LANES), LANES)], left4.at[y, z],
            s_l2.at[d], r_l2.at[d], **{AZ: to},
        )

    def left_step2(d):
        left_copy2(d).start()
        remote(cz.at[z], cz.at[z], s_c.at[1], r_c.at[1], **{AZ: wrap(z + d, NZ)}).start()

    def left_step3(d):
        piece = left4.at[y, wrap(z - d, NZ)]
        for dy in range(1, NY):
            remote(piece, piece, s_l3.at[dy], r_l3.at[dy], **{AY: wrap(y + dy, NY)}).start()

    def left_wait3():
        rest = cz.at[pl.ds(0, NZ - 1)]
        remote(rest, rest, s_c.at[1], r_c.at[1], **{AZ: wrap(z + 1, NZ)}).wait()
        for dy in range(1, NY):
            remote(left4.at[y], left4.at[wrap(y - dy, NY)], s_l3.at[dy], r_l3.at[dy], **{AY: wrap(y + dy, NY)}).wait()

    low = lax.div(7 * z, 2)
    off = pl.multiple_of(lax.rem(z, 2) * (LANES // 2), LANES // 2)
    k_all = NZ * NX * slab

    def transpose_left():
        for p in range(NY):
            yp = lax.rem(low + p, NY)
            for s in range(NZ):
                left[p * LANES:(p + 1) * LANES, s * LANES:(s + 1) * LANES] = left4[yp, s].T


    def multiply(c):
        t, a, b, px, pz = spans[c]
        right = jnp.concatenate(
            [gx[:, :, px * LANES:(px + a) * LANES].reshape(k_all, a * LANES),
             gz[:, :, pz * LANES:(pz + b) * LANES].reshape(k_all, b * LANES)], axis=1)
        prod[:, :(a + b) * LANES] = jnp.dot(
            left[pl.ds(off, NY * rows), :], right, preferred_element_type=jnp.float32)

    def send_out(c, to):
        t, a, b, _, _ = spans[c]
        for j in range(t, t + a + b):
            remote(
                code.at[to, :, pl.ds(j * LANES, LANES)], codes.at[:, lanes_of(j * NY + y)],
                s_o.at[c, 0], r_o.at[c, 0], **{AY: to},
            ).start()
        remote(scale.at[to, pl.ds(t, a + b)], scales.at[pl.ds(t, a + b), y], s_o.at[c, 1], r_o.at[c, 1], **{AY: to}).start()

    def encode(c, low, high):
        t, a, b, _, _ = spans[c]
        w = (a + b) * LANES
        factor = 2.0 / jnp.sum(cz[:, 0:1, 0:1], axis=0)

        def one(i, carry):
            to = lax.rem(y + i + 1, NY)
            v = prod[pl.ds(pl.multiple_of(to * rows, 16), rows), :w]
            m = jnp.max(jnp.abs(v), axis=0, keepdims=True)
            r = jnp.where(m > 0.0, 1.0 / jnp.where(m > 0.0, m, 1.0), 0.0)
            u = (jnp.sqrt(jnp.abs(v) * r) * TOP_CODE + 0.5).astype(jnp.int32)
            code[to, :, t * LANES:t * LANES + w] = jnp.where(v < 0.0, -u, u).astype(jnp.int16)
            m = m * factor
            for j in range(a + b):
                scale[to, t + j] = m[:, j * LANES:(j + 1) * LANES]

            @pl.when(i > 0)
            def _():
                send_out(c, lax.rem(y + i, NY))

            return carry

        lax.fori_loop(low, high, one, 0)
        if high == NY:
            for j in range(t, t + a + b):
                codes[:, lanes_of(j * NY + y)] = code[y, :, j * LANES:(j + 1) * LANES]
                scales[j, y] = scale[y, j]

    def lanes_of(tile):
        return pl.ds(pl.multiple_of(tile * LANES, LANES), LANES)

    def receive(c):
        k = (NY - 1) * (spans[c][1] + spans[c][2])
        to = wrap(y + 1, NY)
        whole = codes.at[:, pl.ds(0, k * LANES)]
        remote(whole, whole, s_o.at[c, 0], r_o.at[c, 0], **{AY: to}).wait()
        sizes = scales.at[pl.ds(0, k), 0]
        remote(sizes, sizes, s_o.at[c, 1], r_o.at[c, 1], **{AY: to}).wait()

    waited = False
    for kind, c, d in ORDER:
        if kind in ("l2", "l3") and not waited:
            left_wait1()
            waited = True
        if kind == "l1":
            left_step1()
        elif kind == "l2":
            for way in sorted({d, NZ - d}):
                left_step2(way)
        elif kind == "l3":
            for way in sorted({d, (NZ - d) % NZ}):
                if d:
                    left_copy2(way).wait()
                left_step3(way)
        elif kind == "mm":
            if d == 1:
                rings[c][1].finish()
                rings[c][3].finish()
                if c == 0:
                    left_wait3()
                    transpose_left()
                multiply(c)
            else:
                encode(c, *((0, NY // 2) if d == 2 else (NY // 2, NY)))
        else:
            k = ("px", "pz", "qz", "qx").index(kind)
            if d == 1 and k in (1, 3):
                rings[c][k - 1].finish()
            rings[c][k].run(d)
    for c in range(len(CHUNKS)):
        receive(c)


def exchange(acts, ids):
    n = len(CHUNKS)
    tiles = sum(a + b for a, b in CHUNKS)
    t_x, t_z = (sum(c[i] for c in CHUNKS) for i in (0, 1))
    slab = NY * NE * CAP
    wide = max(a + b for a, b in CHUNKS) * LANES
    rows = tiles * LANES // (NX * NZ)
    bf16, f32, i16 = jnp.bfloat16, jnp.float32, jnp.int16
    dma = pltpu.SemaphoreType.DMA
    vmem = pl.BlockSpec(memory_space=pltpu.VMEM)
    return pl.pallas_call(
        kernel,
        out_shape=(
            jax.ShapeDtypeStruct((rows, tiles * NY * LANES), i16),
            jax.ShapeDtypeStruct((tiles, NY, 1, LANES), f32),
        ),
        in_specs=[vmem, vmem],
        out_specs=(vmem, vmem),
        scratch_shapes=[
            pltpu.VMEM((NY * NE, CAP, (tiles + 1) * LANES), bf16),
            pltpu.VMEM((NE * CAP, tiles * NY * LANES), f32),
            pltpu.VMEM((NY * NE, CAP, (tiles + 1) * LANES), bf16),
            pltpu.VMEM((slab, tiles * LANES), bf16),
            pltpu.VMEM((NX * slab, tiles * LANES // NX), bf16),
            pltpu.VMEM((NY, NZ, NX * slab, LANES), bf16),
            pltpu.VMEM((NY * LANES, NZ * NX * slab), bf16),
            pltpu.VMEM((NZ, NX * slab, t_x * LANES), bf16),
            pltpu.VMEM((NZ, NX * slab, t_z * LANES), bf16),
            pltpu.VMEM((NY * rows, wide), f32),
            pltpu.VMEM((NY, rows, tiles * LANES), i16),
            pltpu.VMEM((NY, tiles, 1, LANES), f32),
            pltpu.VMEM((NX, 8, LANES), f32),
            pltpu.VMEM((NZ, 8, LANES), f32),
            dma(()), dma(()),
            dma((2,)), dma((2,)),
            dma(()), dma(()),
            dma((NZ,)), dma((NZ,)),
            dma((NY,)), dma((NY,)),
            dma((n,)), dma((n,)),
            dma((n,)), dma((n, NZ // 2)),
            dma((n,)), dma((n, NZ // 2)),
            dma((n,)), dma((n, NX // 2)),
            dma((max(DIRECT, 1),)), dma((max(DIRECT, 1),)),
            dma((n, 2)), dma((n, 2)),
        ],
        compiler_params=pltpu.CompilerParams(
            collective_id=0, has_side_effects=True, vmem_limit_bytes=48 * 1024 * 1024
        ),
        name="exchange",
    )(acts, ids)


def shards(activations, expert_ids):
    ff = activations.shape[1]
    codes, scales = exchange(activations, expert_ids)
    u = codes.astype(jnp.float32) * (1.0 / TOP_CODE)
    return (u * jnp.abs(u) * scales.reshape(1, ff))[None]


def solution(mesh):
    split = Mesh(mesh.devices.reshape(NX, NZ, NY, NE), TOK_EXP)
    return jax.shard_map(
        shards,
        mesh=split,
        in_specs=(P(TOK_EXP, None), P(TOK_EXP, None)),
        out_specs=P(AE, TOK, None),
        check_vma=False,
    )
```

```python
import functools

import jax
import jax.numpy as jnp
from jax import lax
from jax.experimental import pallas as pl
from jax.experimental.pallas import tpu as pltpu
from jax.sharding import Mesh
from jax.sharding import PartitionSpec as P

CAP = 4
LANES = 128
AX, AZ, AY, AE = "tok_0", "tok_1", "tok_2", "exp"
TOK = (AX, AZ, AY)
TOK_EXP = (AX, AZ, AY, AE)
NX, NZ, NY, NE = 4, 8, 4, 2
TOP_CODE = 32767.0

CHUNKS = ((1, 1), (1, 2), (1, 3), (2, 3), (1, 2), (1, 2), (1, 2), (4, 1))
DIRECT = 1
ORDER = (
    ("px", 0, 1), ("px", 1, 1), ("px", 5, 1), ("l1", 0, 1), ("qz", 1, 1), ("qz", 2, 1), ("qz", 4, 1), ("qz", 0, 1),
    ("px", 7, 1), ("qz", 3, 1), ("px", 2, 1), ("px", 4, 1), ("qz", 1, 2), ("px", 3, 1), ("pz", 0, 1), ("px", 6, 1),
    ("pz", 1, 1), ("qz", 4, 2), ("qz", 2, 2), ("qz", 7, 1), ("qz", 3, 2), ("qz", 1, 3), ("l3", 0, 0), ("l2", 0, 2),
    ("qx", 0, 1), ("l2", 0, 1), ("qz", 2, 3), ("l2", 0, 4), ("qz", 1, 4), ("pz", 0, 2), ("qx", 0, 2), ("l3", 0, 2),
    ("l3", 0, 1), ("l2", 0, 3), ("qx", 1, 1), ("qz", 3, 3), ("qz", 2, 4), ("pz", 0, 3), ("pz", 1, 2), ("l3", 0, 4),
    ("qz", 4, 3), ("pz", 2, 1), ("qz", 3, 4), ("qx", 2, 1), ("qz", 5, 1), ("qz", 6, 1), ("l3", 0, 3), ("pz", 0, 4),
    ("pz", 3, 1), ("qx", 1, 2), ("pz", 1, 3), ("qz", 4, 4), ("qx", 3, 1), ("pz", 2, 2), ("pz", 4, 1), ("qz", 6, 2),
    ("qz", 5, 2), ("pz", 3, 2), ("pz", 1, 4), ("mm", 0, 1), ("pz", 2, 3), ("qx", 2, 2), ("mm", 0, 2), ("qz", 5, 3),
    ("mm", 0, 3), ("qz", 6, 3), ("pz", 5, 1), ("qx", 4, 1), ("pz", 3, 3), ("mm", 1, 1), ("mm", 1, 2), ("mm", 1, 3),
    ("pz", 2, 4), ("qz", 5, 4), ("qz", 6, 4), ("qz", 7, 2), ("pz", 4, 2), ("qx", 3, 2), ("pz", 5, 2), ("pz", 6, 1),
    ("pz", 3, 4), ("mm", 2, 1), ("qz", 7, 3), ("qx", 5, 1), ("mm", 2, 2), ("pz", 4, 3), ("mm", 2, 3), ("pz", 5, 3),
    ("pz", 7, 1), ("qx", 4, 2), ("qx", 6, 1), ("mm", 3, 1), ("qz", 7, 4), ("pz", 5, 4), ("mm", 3, 2), ("pz", 4, 4),
    ("mm", 3, 3), ("pz", 6, 2), ("qx", 5, 2), ("pz", 7, 2), ("qx", 7, 1), ("mm", 4, 1), ("mm", 4, 2), ("mm", 4, 3),
    ("pz", 6, 3), ("qx", 6, 2), ("pz", 7, 3), ("mm", 5, 1), ("mm", 5, 2), ("mm", 5, 3), ("qx", 7, 2), ("pz", 6, 4),
    ("pz", 7, 4), ("mm", 6, 1), ("mm", 6, 2), ("mm", 6, 3), ("mm", 7, 1), ("mm", 7, 2), ("mm", 7, 3),
)


def place_tokens(acts, ids, slots, chosen):
    named = ids[...]
    n = named.shape[0]
    row = lax.broadcasted_iota(jnp.int32, (n, n), 0)
    column = lax.broadcasted_iota(jnp.int32, (n, n), 1)
    slot = lax.broadcasted_iota(jnp.int32, (CAP, n), 0).astype(jnp.float32)
    picks = []
    for e in range(NE):
        routed = jnp.max(jnp.where(named == e, 1.0, 0.0), axis=1, keepdims=True)
        rank = jnp.sum(jnp.where(row < column, routed, 0.0), axis=0, keepdims=True)
        here = jnp.sum(jnp.where(row == column, routed, 0.0), axis=0, keepdims=True)
        picks.append(jnp.where((rank == slot) & (here > 0.0), 1.0, 0.0))
    width = slots.shape[2] - LANES
    pick = jnp.concatenate(picks, axis=0).astype(jnp.bfloat16)
    chosen[...] = jnp.dot(pick, acts[...], preferred_element_type=jnp.float32)
    for e in range(NE):
        mark = jnp.broadcast_to(jnp.sum(picks[e], axis=1, keepdims=True), (CAP, LANES)).astype(jnp.bfloat16)
        for y in range(NY):
            slots[y * NE + e, :, :width] = jnp.concatenate(
                [chosen[e * CAP:(e + 1) * CAP, (j * NY + y) * LANES:(j * NY + y + 1) * LANES] for j in range(width // LANES)],
                axis=1,
            ).astype(jnp.bfloat16)
            slots[y * NE + e, :, width:] = mark


def remote(src, dst, send, recv, **where):
    return pltpu.make_async_remote_copy(
        src_ref=src,
        dst_ref=dst,
        send_sem=send,
        recv_sem=recv,
        device_id=where,
        device_id_type=pl.DeviceIdType.MESH,
    )


def wrap(index, count):
    return lax.rem(index + count, count)


class Ring:
    def __init__(self, axis, count, view, extent, send, recv, two):
        self.axis, self.count, self.view, self.extent = axis, count, view, extent
        self.send, self.recv, self.two = send, recv, two
        self.me = lax.axis_index(axis)
        self.steps = count // 2

    def wait(self, step):
        ref = self.two if step < self.steps else self.view(self.me, 0, self.extent)
        to = wrap(self.me + 1, self.count)
        remote(ref, ref, self.send, self.recv.at[step - 1], **{self.axis: to}).wait()

    def run(self, step):
        if step > 1:
            self.wait(step - 1)
        half = self.extent // 2
        for way, sign in enumerate((1, -1)):
            at, size = (way * half, half) if step == self.steps else (0, self.extent)
            ref = self.view(wrap(self.me - sign * (step - 1), self.count), at, size)
            to = wrap(self.me + sign, self.count)
            remote(ref, ref, self.send, self.recv.at[step - 1], **{self.axis: to}).start()

    def finish(self):
        self.wait(self.steps)


class Direct:
    def __init__(self, axis, count, view, extent, send, recv, others):
        self.axis, self.count, self.view, self.extent = axis, count, view, extent
        self.send, self.recv, self.others = send, recv, others
        self.me = lax.axis_index(axis)
        self.steps = 1

    def run(self, step):
        ref = self.view(self.me, 0, self.extent)
        for d in sorted(range(1, self.count), key=lambda d: min(d, self.count - d)):
            to = wrap(self.me + d, self.count)
            remote(ref, ref, self.send, self.recv, **{self.axis: to}).start()

    def finish(self):
        remote(self.others, self.others, self.send, self.recv, **{self.axis: wrap(self.me + 1, self.count)}).wait()


def kernel(
    acts, ids, codes, scales,
    slots, chosen, arrived, own, left1, left4, left, gx, gz, prod, code, scale, cx, cz,
    s_y, r_y, s_c, r_c, s_l1, r_l1, s_l2, r_l2, s_l3, r_l3,
    s_xf, r_xf, s_zs, r_zs, s_zf, r_zf, s_xs, r_xs, s_zd, r_zd, s_o, r_o,
):
    x, z, y, e = (lax.axis_index(a) for a in (AX, AZ, AY, AE))
    rows = prod.shape[0] // NY
    slab = NY * NE * CAP
    marks_at = own.shape[1]

    pairs = [(dy, de) for dy in range(NY) for de in range(NE) if (dy, de) != (0, 0)]
    barrier = pltpu.get_barrier_semaphore()
    for d in range(1, NX):
        pl.semaphore_signal(barrier, inc=1, device_id={AX: wrap(x + d, NX)}, device_id_type=pl.DeviceIdType.MESH)
    for d in range(1, NZ):
        pl.semaphore_signal(barrier, inc=1, device_id={AZ: wrap(z + d, NZ)}, device_id_type=pl.DeviceIdType.MESH)
    for dy, de in pairs:
        pl.semaphore_signal(barrier, inc=1, device_id={AY: wrap(y + dy, NY), AE: wrap(e + de, NE)}, device_id_type=pl.DeviceIdType.MESH)
    place_tokens(acts, ids, slots, chosen)
    pl.semaphore_wait(barrier, NX - 1 + NZ - 1 + len(pairs))

    me = y * NE + e
    for dy, de in pairs:
        ty, te = wrap(y + dy, NY), wrap(e + de, NE)
        remote(slots.at[ty * NE + te], arrived.at[me], s_y, r_y, **{AY: ty, AE: te}).start()
    arrived[me] = slots[me]
    most = pl.ds(0, len(pairs))
    remote(slots.at[most], arrived.at[most], s_y, r_y, **{AE: wrap(e + 1, NE)}).wait()

    mine = jnp.concatenate(
        [arrived[i, :, :marks_at].astype(jnp.float32) for i in range(NY * NE)], axis=0
    ).astype(jnp.bfloat16)
    own[...] = mine
    at_x = pl.ds(pl.multiple_of(x * slab, slab), slab)
    tile = 0
    spans = []
    px = pz = 0
    for a, b in CHUNKS:
        gx[z, at_x, px * LANES:(px + a) * LANES] = own[:, tile * LANES:(tile + a) * LANES]
        gz[z, at_x, pz * LANES:(pz + b) * LANES] = own[:, (tile + a) * LANES:(tile + a + b) * LANES]
        spans.append((tile, a, b, px, pz))
        tile, px, pz = tile + a + b, px + a, pz + b
    left1[at_x, :] = own[:, pl.ds(pl.multiple_of(x * left1.shape[1], LANES), left1.shape[1])]
    marks = sum(
        jnp.sum(arrived[i, :, marks_at:].astype(jnp.float32), axis=0, keepdims=True)
        for i in range(NY * NE)
    )
    cx[x] = jnp.broadcast_to(marks, cx.shape[1:])

    def rows_of(block, at, size):
        return pl.ds(pl.multiple_of(block * slab + at, 8), size)

    rings = []
    for c, (_, a, b, px, pz) in enumerate(spans):
        on_x, on_z = pl.ds(px * LANES, a * LANES), pl.ds(pz * LANES, b * LANES)
        rings.append((
            Direct(AX, NX, lambda k, at, m, w=on_x: gx.at[z, rows_of(k, at, m), w], slab, s_xf.at[c], r_xf.at[c],
                   gx.at[z, pl.ds(0, (NX - 1) * slab), on_x]),
            Ring(AZ, NZ, lambda k, at, m, w=on_x: gx.at[k, pl.ds(at, m), w], NX * slab, s_zs.at[c], r_zs.at[c],
                 gx.at[pl.ds(0, 2), :, on_x]),
            Direct(AZ, NZ, lambda k, at, m, w=on_z: gz.at[k, rows_of(x, at, m), w], slab, s_zd.at[c], r_zd.at[c],
                   gz.at[pl.ds(0, NZ - 1), at_x, on_z])
            if c < DIRECT else
            Ring(AZ, NZ, lambda k, at, m, w=on_z: gz.at[k, rows_of(x, at, m), w], slab, s_zf.at[c], r_zf.at[c],
                 gz.at[pl.ds(0, 2), at_x, on_z]),
            Ring(AX, NX, lambda k, at, m, w=on_z: gz.at[pl.ds(at, m), rows_of(k, 0, slab), w], NZ, s_xs.at[c], r_xs.at[c],
                 gz.at[:, pl.ds(0, 2 * slab), on_z]),
        ))

    def left_step1():
        w = left1.shape[1]
        for d in range(1, NX):
            to = wrap(x + d, NX)
            remote(
                own.at[:, pl.ds(pl.multiple_of(to * w, LANES), w)], left1.at[at_x, :], s_l1, r_l1, **{AX: to}
            ).start()
            remote(cx.at[x], cx.at[x], s_c.at[0], r_c.at[0], **{AX: to}).start()

    def left_wait1():
        w, k = left1.shape[1], (NX - 1) * slab
        to = wrap(x + 1, NX)
        remote(own.at[:, pl.ds(0, (NX - 1) * w)], left1.at[pl.ds(0, k), :], s_l1, r_l1, **{AX: to}).wait()
        rest = cx.at[pl.ds(0, NX - 1)]
        remote(rest, rest, s_c.at[0], r_c.at[0], **{AX: to}).wait()
        cz[z] = sum(cx[i] for i in range(NX))
        left4[y, z] = left1[:, pl.ds(pl.multiple_of(local_tile(z) * LANES, LANES), LANES)]

    def local_tile(zz):
        return lax.div(lax.div(7 * zz, 2) - y + (NY - 1), NY)

    def left_copy2(d):
        to = wrap(z + d, NZ)
        return remote(
            left1.at[:, pl.ds(pl.multiple_of(local_tile(to) * LANES, LANES), LANES)], left4.at[y, z],
            s_l2.at[d], r_l2.at[d], **{AZ: to},
        )

    def left_step2(d):
        left_copy2(d).start()
        remote(cz.at[z], cz.at[z], s_c.at[1], r_c.at[1], **{AZ: wrap(z + d, NZ)}).start()

    def left_step3(d):
        piece = left4.at[y, wrap(z - d, NZ)]
        for dy in range(1, NY):
            remote(piece, piece, s_l3.at[dy], r_l3.at[dy], **{AY: wrap(y + dy, NY)}).start()

    def left_wait3():
        rest = cz.at[pl.ds(0, NZ - 1)]
        remote(rest, rest, s_c.at[1], r_c.at[1], **{AZ: wrap(z + 1, NZ)}).wait()
        for dy in range(1, NY):
            remote(left4.at[y], left4.at[wrap(y - dy, NY)], s_l3.at[dy], r_l3.at[dy], **{AY: wrap(y + dy, NY)}).wait()

    low = lax.div(7 * z, 2)
    off = pl.multiple_of(lax.rem(z, 2) * (LANES // 2), LANES // 2)
    k_all = NZ * NX * slab

    def transpose_left():
        for p in range(NY):
            yp = lax.rem(low + p, NY)
            for s in range(NZ):
                left[p * LANES:(p + 1) * LANES, s * LANES:(s + 1) * LANES] = left4[yp, s].T


    def multiply(c):
        t, a, b, px, pz = spans[c]
        right = jnp.concatenate(
            [gx[:, :, px * LANES:(px + a) * LANES].reshape(k_all, a * LANES),
             gz[:, :, pz * LANES:(pz + b) * LANES].reshape(k_all, b * LANES)], axis=1)
        prod[:, :(a + b) * LANES] = jnp.dot(
            left[pl.ds(off, NY * rows), :], right, preferred_element_type=jnp.float32)

    def send_out(c, to):
        t, a, b, _, _ = spans[c]
        for j in range(t, t + a + b):
            remote(
                code.at[to, :, pl.ds(j * LANES, LANES)], codes.at[:, lanes_of(j * NY + y)],
                s_o.at[c, 0], r_o.at[c, 0], **{AY: to},
            ).start()
        remote(scale.at[to, pl.ds(t, a + b)], scales.at[pl.ds(t, a + b), y], s_o.at[c, 1], r_o.at[c, 1], **{AY: to}).start()

    def encode(c, low, high):
        t, a, b, _, _ = spans[c]
        w = (a + b) * LANES
        factor = 2.0 / jnp.sum(cz[:, 0:1, 0:1], axis=0)

        def one(i, carry):
            to = lax.rem(y + i + 1, NY)
            v = prod[pl.ds(pl.multiple_of(to * rows, 16), rows), :w]
            m = jnp.max(jnp.abs(v), axis=0, keepdims=True)
            r = jnp.where(m > 0.0, 1.0 / jnp.where(m > 0.0, m, 1.0), 0.0)
            u = (jnp.sqrt(jnp.abs(v) * r) * TOP_CODE + 0.5).astype(jnp.int32)
            code[to, :, t * LANES:t * LANES + w] = jnp.where(v < 0.0, -u, u).astype(jnp.int16)
            m = m * factor
            for j in range(a + b):
                scale[to, t + j] = m[:, j * LANES:(j + 1) * LANES]

            @pl.when(i > 0)
            def _():
                send_out(c, lax.rem(y + i, NY))

            return carry

        lax.fori_loop(low, high, one, 0)
        if high == NY:
            for j in range(t, t + a + b):
                codes[:, lanes_of(j * NY + y)] = code[y, :, j * LANES:(j + 1) * LANES]
                scales[j, y] = scale[y, j]

    def lanes_of(tile):
        return pl.ds(pl.multiple_of(tile * LANES, LANES), LANES)

    def receive(c):
        k = (NY - 1) * (spans[c][1] + spans[c][2])
        to = wrap(y + 1, NY)
        whole = codes.at[:, pl.ds(0, k * LANES)]
        remote(whole, whole, s_o.at[c, 0], r_o.at[c, 0], **{AY: to}).wait()
        sizes = scales.at[pl.ds(0, k), 0]
        remote(sizes, sizes, s_o.at[c, 1], r_o.at[c, 1], **{AY: to}).wait()

    waited = False
    for kind, c, d in ORDER:
        if kind in ("l2", "l3") and not waited:
            left_wait1()
            waited = True
        if kind == "l1":
            left_step1()
        elif kind == "l2":
            for way in sorted({d, NZ - d}):
                left_step2(way)
        elif kind == "l3":
            for way in sorted({d, (NZ - d) % NZ}):
                if d:
                    left_copy2(way).wait()
                left_step3(way)
        elif kind == "mm":
            if d == 1:
                rings[c][1].finish()
                rings[c][3].finish()
                if c == 0:
                    left_wait3()
                    transpose_left()
                multiply(c)
            else:
                encode(c, *((0, NY // 2) if d == 2 else (NY // 2, NY)))
        else:
            k = ("px", "pz", "qz", "qx").index(kind)
            if d == 1 and k in (1, 3):
                rings[c][k - 1].finish()
            rings[c][k].run(d)
    for c in range(len(CHUNKS)):
        receive(c)


def exchange(acts, ids):
    n = len(CHUNKS)
    tiles = sum(a + b for a, b in CHUNKS)
    t_x, t_z = (sum(c[i] for c in CHUNKS) for i in (0, 1))
    slab = NY * NE * CAP
    wide = max(a + b for a, b in CHUNKS) * LANES
    rows = tiles * LANES // (NX * NZ)
    bf16, f32, i16 = jnp.bfloat16, jnp.float32, jnp.int16
    dma = pltpu.SemaphoreType.DMA
    vmem = pl.BlockSpec(memory_space=pltpu.VMEM)
    return pl.pallas_call(
        kernel,
        out_shape=(
            jax.ShapeDtypeStruct((rows, tiles * NY * LANES), i16),
            jax.ShapeDtypeStruct((tiles, NY, 1, LANES), f32),
        ),
        in_specs=[vmem, vmem],
        out_specs=(vmem, vmem),
        scratch_shapes=[
            pltpu.VMEM((NY * NE, CAP, (tiles + 1) * LANES), bf16),
            pltpu.VMEM((NE * CAP, tiles * NY * LANES), f32),
            pltpu.VMEM((NY * NE, CAP, (tiles + 1) * LANES), bf16),
            pltpu.VMEM((slab, tiles * LANES), bf16),
            pltpu.VMEM((NX * slab, tiles * LANES // NX), bf16),
            pltpu.VMEM((NY, NZ, NX * slab, LANES), bf16),
            pltpu.VMEM((NY * LANES, NZ * NX * slab), bf16),
            pltpu.VMEM((NZ, NX * slab, t_x * LANES), bf16),
            pltpu.VMEM((NZ, NX * slab, t_z * LANES), bf16),
            pltpu.VMEM((NY * rows, wide), f32),
            pltpu.VMEM((NY, rows, tiles * LANES), i16),
            pltpu.VMEM((NY, tiles, 1, LANES), f32),
            pltpu.VMEM((NX, 8, LANES), f32),
            pltpu.VMEM((NZ, 8, LANES), f32),
            dma(()), dma(()),
            dma((2,)), dma((2,)),
            dma(()), dma(()),
            dma((NZ,)), dma((NZ,)),
            dma((NY,)), dma((NY,)),
            dma((n,)), dma((n,)),
            dma((n,)), dma((n, NZ // 2)),
            dma((n,)), dma((n, NZ // 2)),
            dma((n,)), dma((n, NX // 2)),
            dma((max(DIRECT, 1),)), dma((max(DIRECT, 1),)),
            dma((n, 2)), dma((n, 2)),
        ],
        compiler_params=pltpu.CompilerParams(
            collective_id=0, has_side_effects=True, vmem_limit_bytes=48 * 1024 * 1024
        ),
        name="exchange",
    )(acts, ids)


def shards(activations, expert_ids):
    ff = activations.shape[1]
    codes, scales = exchange(activations, expert_ids)
    u = codes.astype(jnp.float32) * (1.0 / TOP_CODE)
    return (u * jnp.abs(u) * scales.reshape(1, ff))[None]


def solution(mesh):
    split = Mesh(mesh.devices.reshape(NX, NZ, NY, NE), TOK_EXP)
    return jax.shard_map(
        shards,
        mesh=split,
        in_specs=(P(TOK_EXP, None), P(TOK_EXP, None)),
        out_specs=P(AE, TOK, None),
        check_vma=False,
    )
```

```python
import functools

import jax
import jax.numpy as jnp
from jax import lax
from jax.experimental import pallas as pl
from jax.experimental.pallas import tpu as pltpu
from jax.sharding import Mesh
from jax.sharding import PartitionSpec as P

CAP = 4
LANES = 128
AX, AZ, AY, AE = "tok_0", "tok_1", "tok_2", "exp"
TOK = (AX, AZ, AY)
TOK_EXP = (AX, AZ, AY, AE)
NX, NZ, NY, NE = 4, 8, 4, 2
TOP_CODE = 32767.0

CHUNKS = ((2, 2), (1, 2), (1, 1), (1, 2), (1, 2), (2, 2), (2, 2), (3, 2))
DIRECT = 0
ORDER = (
    ("qz", 2, 1), ("l1", 0, 1), ("px", 5, 1), ("qz", 5, 1), ("px", 0, 1), ("px", 3, 1), ("qz", 0, 1), ("px", 1, 1),
    ("px", 2, 1), ("px", 6, 1), ("qz", 3, 1), ("px", 7, 1), ("px", 4, 1), ("qz", 1, 1), ("qz", 7, 1), ("qz", 4, 1),
    ("qz", 6, 1), ("qz", 2, 2), ("qz", 5, 2), ("qz", 0, 2), ("qz", 3, 2), ("qz", 1, 2), ("qz", 7, 2), ("qz", 4, 2),
    ("qz", 6, 2), ("qz", 2, 3), ("l2", 0, 4), ("l3", 0, 0), ("qz", 0, 3), ("qz", 1, 3), ("l2", 0, 1), ("qz", 4, 3),
    ("qz", 2, 4), ("pz", 0, 1), ("qz", 0, 4), ("l2", 0, 3), ("l3", 0, 1), ("qx", 2, 1), ("l3", 0, 4), ("qz", 1, 4),
    ("pz", 4, 1), ("qx", 0, 1), ("pz", 0, 2), ("l2", 0, 2), ("qx", 2, 2), ("qx", 1, 1), ("qz", 4, 4), ("pz", 1, 1),
    ("l3", 0, 3), ("qz", 3, 3), ("qz", 6, 3), ("pz", 0, 3), ("qx", 0, 2), ("qx", 4, 1), ("pz", 3, 1), ("l3", 0, 2),
    ("pz", 1, 2), ("qz", 3, 4), ("qz", 6, 4), ("pz", 2, 1), ("pz", 4, 2), ("qx", 1, 2), ("pz", 0, 4), ("pz", 3, 2),
    ("qx", 3, 1), ("qx", 6, 1), ("pz", 1, 3), ("pz", 2, 2), ("qz", 5, 3), ("pz", 5, 1), ("mm", 0, 1), ("mm", 0, 2),
    ("pz", 1, 4), ("pz", 3, 3), ("mm", 0, 3), ("pz", 2, 3), ("qx", 4, 2), ("qz", 5, 4), ("pz", 4, 3), ("qz", 7, 3),
    ("pz", 5, 2), ("mm", 1, 1), ("qx", 3, 2), ("mm", 1, 2), ("mm", 1, 3), ("pz", 2, 4), ("pz", 3, 4), ("qx", 5, 1),
    ("pz", 6, 1), ("qx", 6, 2), ("pz", 4, 4), ("qz", 7, 4), ("pz", 7, 1), ("mm", 2, 1), ("mm", 2, 2), ("mm", 2, 3),
    ("mm", 3, 1), ("pz", 5, 3), ("mm", 3, 2), ("qx", 7, 1), ("mm", 3, 3), ("pz", 6, 2), ("mm", 4, 1), ("mm", 4, 2),
    ("mm", 4, 3), ("pz", 7, 2), ("qx", 5, 2), ("pz", 5, 4), ("pz", 6, 3), ("qx", 7, 2), ("pz", 7, 3), ("mm", 5, 1),
    ("mm", 5, 2), ("mm", 5, 3), ("pz", 6, 4), ("pz", 7, 4), ("mm", 6, 1), ("mm", 6, 2), ("mm", 6, 3), ("mm", 7, 1),
    ("mm", 7, 2), ("mm", 7, 3),
)


def place_tokens(acts, ids, slots, chosen):
    named = ids[...]
    n = named.shape[0]
    row = lax.broadcasted_iota(jnp.int32, (n, n), 0)
    column = lax.broadcasted_iota(jnp.int32, (n, n), 1)
    slot = lax.broadcasted_iota(jnp.int32, (CAP, n), 0).astype(jnp.float32)
    picks = []
    for e in range(NE):
        routed = jnp.max(jnp.where(named == e, 1.0, 0.0), axis=1, keepdims=True)
        rank = jnp.sum(jnp.where(row < column, routed, 0.0), axis=0, keepdims=True)
        here = jnp.sum(jnp.where(row == column, routed, 0.0), axis=0, keepdims=True)
        picks.append(jnp.where((rank == slot) & (here > 0.0), 1.0, 0.0))
    width = slots.shape[2] - LANES
    pick = jnp.concatenate(picks, axis=0).astype(jnp.bfloat16)
    chosen[...] = jnp.dot(pick, acts[...], preferred_element_type=jnp.float32)
    for e in range(NE):
        mark = jnp.broadcast_to(jnp.sum(picks[e], axis=1, keepdims=True), (CAP, LANES)).astype(jnp.bfloat16)
        for y in range(NY):
            slots[y * NE + e, :, :width] = jnp.concatenate(
                [chosen[e * CAP:(e + 1) * CAP, (j * NY + y) * LANES:(j * NY + y + 1) * LANES] for j in range(width // LANES)],
                axis=1,
            ).astype(jnp.bfloat16)
            slots[y * NE + e, :, width:] = mark


def remote(src, dst, send, recv, **where):
    return pltpu.make_async_remote_copy(
        src_ref=src,
        dst_ref=dst,
        send_sem=send,
        recv_sem=recv,
        device_id=where,
        device_id_type=pl.DeviceIdType.MESH,
    )


def wrap(index, count):
    return lax.rem(index + count, count)


class Ring:
    def __init__(self, axis, count, view, extent, send, recv, two):
        self.axis, self.count, self.view, self.extent = axis, count, view, extent
        self.send, self.recv, self.two = send, recv, two
        self.me = lax.axis_index(axis)
        self.steps = count // 2

    def wait(self, step):
        ref = self.two if step < self.steps else self.view(self.me, 0, self.extent)
        to = wrap(self.me + 1, self.count)
        remote(ref, ref, self.send, self.recv.at[step - 1], **{self.axis: to}).wait()

    def run(self, step):
        if step > 1:
            self.wait(step - 1)
        half = self.extent // 2
        for way, sign in enumerate((1, -1)):
            at, size = (way * half, half) if step == self.steps else (0, self.extent)
            ref = self.view(wrap(self.me - sign * (step - 1), self.count), at, size)
            to = wrap(self.me + sign, self.count)
            remote(ref, ref, self.send, self.recv.at[step - 1], **{self.axis: to}).start()

    def finish(self):
        self.wait(self.steps)


class Direct:
    def __init__(self, axis, count, view, extent, send, recv, others):
        self.axis, self.count, self.view, self.extent = axis, count, view, extent
        self.send, self.recv, self.others = send, recv, others
        self.me = lax.axis_index(axis)
        self.steps = 1

    def run(self, step):
        ref = self.view(self.me, 0, self.extent)
        for d in sorted(range(1, self.count), key=lambda d: min(d, self.count - d)):
            to = wrap(self.me + d, self.count)
            remote(ref, ref, self.send, self.recv, **{self.axis: to}).start()

    def finish(self):
        remote(self.others, self.others, self.send, self.recv, **{self.axis: wrap(self.me + 1, self.count)}).wait()


def kernel(
    acts, ids, codes, scales,
    slots, chosen, arrived, own, left1, left4, left, gx, gz, prod, code, scale, cx, cz,
    s_y, r_y, s_c, r_c, s_l1, r_l1, s_l2, r_l2, s_l3, r_l3,
    s_xf, r_xf, s_zs, r_zs, s_zf, r_zf, s_xs, r_xs, s_zd, r_zd, s_o, r_o,
):
    x, z, y, e = (lax.axis_index(a) for a in (AX, AZ, AY, AE))
    rows = prod.shape[0] // NY
    slab = NY * NE * CAP
    marks_at = own.shape[1]

    pairs = [(dy, de) for dy in range(NY) for de in range(NE) if (dy, de) != (0, 0)]
    barrier = pltpu.get_barrier_semaphore()
    for d in range(1, NX):
        pl.semaphore_signal(barrier, inc=1, device_id={AX: wrap(x + d, NX)}, device_id_type=pl.DeviceIdType.MESH)
    for d in range(1, NZ):
        pl.semaphore_signal(barrier, inc=1, device_id={AZ: wrap(z + d, NZ)}, device_id_type=pl.DeviceIdType.MESH)
    for dy, de in pairs:
        pl.semaphore_signal(barrier, inc=1, device_id={AY: wrap(y + dy, NY), AE: wrap(e + de, NE)}, device_id_type=pl.DeviceIdType.MESH)
    place_tokens(acts, ids, slots, chosen)
    pl.semaphore_wait(barrier, NX - 1 + NZ - 1 + len(pairs))

    me = y * NE + e
    for dy, de in pairs:
        ty, te = wrap(y + dy, NY), wrap(e + de, NE)
        remote(slots.at[ty * NE + te], arrived.at[me], s_y, r_y, **{AY: ty, AE: te}).start()
    arrived[me] = slots[me]
    most = pl.ds(0, len(pairs))
    remote(slots.at[most], arrived.at[most], s_y, r_y, **{AE: wrap(e + 1, NE)}).wait()

    mine = jnp.concatenate(
        [arrived[i, :, :marks_at].astype(jnp.float32) for i in range(NY * NE)], axis=0
    ).astype(jnp.bfloat16)
    own[...] = mine
    at_x = pl.ds(pl.multiple_of(x * slab, slab), slab)
    tile = 0
    spans = []
    px = pz = 0
    for a, b in CHUNKS:
        gx[z, at_x, px * LANES:(px + a) * LANES] = own[:, tile * LANES:(tile + a) * LANES]
        gz[z, at_x, pz * LANES:(pz + b) * LANES] = own[:, (tile + a) * LANES:(tile + a + b) * LANES]
        spans.append((tile, a, b, px, pz))
        tile, px, pz = tile + a + b, px + a, pz + b
    left1[at_x, :] = own[:, pl.ds(pl.multiple_of(x * left1.shape[1], LANES), left1.shape[1])]
    marks = sum(
        jnp.sum(arrived[i, :, marks_at:].astype(jnp.float32), axis=0, keepdims=True)
        for i in range(NY * NE)
    )
    cx[x] = jnp.broadcast_to(marks, cx.shape[1:])

    def rows_of(block, at, size):
        return pl.ds(pl.multiple_of(block * slab + at, 8), size)

    rings = []
    for c, (_, a, b, px, pz) in enumerate(spans):
        on_x, on_z = pl.ds(px * LANES, a * LANES), pl.ds(pz * LANES, b * LANES)
        rings.append((
            Direct(AX, NX, lambda k, at, m, w=on_x: gx.at[z, rows_of(k, at, m), w], slab, s_xf.at[c], r_xf.at[c],
                   gx.at[z, pl.ds(0, (NX - 1) * slab), on_x]),
            Ring(AZ, NZ, lambda k, at, m, w=on_x: gx.at[k, pl.ds(at, m), w], NX * slab, s_zs.at[c], r_zs.at[c],
                 gx.at[pl.ds(0, 2), :, on_x]),
            Direct(AZ, NZ, lambda k, at, m, w=on_z: gz.at[k, rows_of(x, at, m), w], slab, s_zd.at[c], r_zd.at[c],
                   gz.at[pl.ds(0, NZ - 1), at_x, on_z])
            if c < DIRECT else
            Ring(AZ, NZ, lambda k, at, m, w=on_z: gz.at[k, rows_of(x, at, m), w], slab, s_zf.at[c], r_zf.at[c],
                 gz.at[pl.ds(0, 2), at_x, on_z]),
            Ring(AX, NX, lambda k, at, m, w=on_z: gz.at[pl.ds(at, m), rows_of(k, 0, slab), w], NZ, s_xs.at[c], r_xs.at[c],
                 gz.at[:, pl.ds(0, 2 * slab), on_z]),
        ))

    def left_step1():
        w = left1.shape[1]
        for d in range(1, NX):
            to = wrap(x + d, NX)
            remote(
                own.at[:, pl.ds(pl.multiple_of(to * w, LANES), w)], left1.at[at_x, :], s_l1, r_l1, **{AX: to}
            ).start()
            remote(cx.at[x], cx.at[x], s_c.at[0], r_c.at[0], **{AX: to}).start()

    def left_wait1():
        w, k = left1.shape[1], (NX - 1) * slab
        to = wrap(x + 1, NX)
        remote(own.at[:, pl.ds(0, (NX - 1) * w)], left1.at[pl.ds(0, k), :], s_l1, r_l1, **{AX: to}).wait()
        rest = cx.at[pl.ds(0, NX - 1)]
        remote(rest, rest, s_c.at[0], r_c.at[0], **{AX: to}).wait()
        cz[z] = sum(cx[i] for i in range(NX))
        left4[y, z] = left1[:, pl.ds(pl.multiple_of(local_tile(z) * LANES, LANES), LANES)]

    def local_tile(zz):
        return lax.div(lax.div(7 * zz, 2) - y + (NY - 1), NY)

    def left_copy2(d):
        to = wrap(z + d, NZ)
        return remote(
            left1.at[:, pl.ds(pl.multiple_of(local_tile(to) * LANES, LANES), LANES)], left4.at[y, z],
            s_l2.at[d], r_l2.at[d], **{AZ: to},
        )

    def left_step2(d):
        left_copy2(d).start()
        remote(cz.at[z], cz.at[z], s_c.at[1], r_c.at[1], **{AZ: wrap(z + d, NZ)}).start()

    def left_step3(d):
        piece = left4.at[y, wrap(z - d, NZ)]
        for dy in range(1, NY):
            remote(piece, piece, s_l3.at[dy], r_l3.at[dy], **{AY: wrap(y + dy, NY)}).start()

    def left_wait3():
        rest = cz.at[pl.ds(0, NZ - 1)]
        remote(rest, rest, s_c.at[1], r_c.at[1], **{AZ: wrap(z + 1, NZ)}).wait()
        for dy in range(1, NY):
            remote(left4.at[y], left4.at[wrap(y - dy, NY)], s_l3.at[dy], r_l3.at[dy], **{AY: wrap(y + dy, NY)}).wait()

    low = lax.div(7 * z, 2)
    off = pl.multiple_of(lax.rem(z, 2) * (LANES // 2), LANES // 2)
    k_all = NZ * NX * slab

    def transpose_left():
        for p in range(NY):
            yp = lax.rem(low + p, NY)
            for s in range(NZ):
                left[p * LANES:(p + 1) * LANES, s * LANES:(s + 1) * LANES] = left4[yp, s].T


    def multiply(c):
        t, a, b, px, pz = spans[c]
        right = jnp.concatenate(
            [gx[:, :, px * LANES:(px + a) * LANES].reshape(k_all, a * LANES),
             gz[:, :, pz * LANES:(pz + b) * LANES].reshape(k_all, b * LANES)], axis=1)
        prod[:, :(a + b) * LANES] = jnp.dot(
            left[pl.ds(off, NY * rows), :], right, preferred_element_type=jnp.float32)

    def send_out(c, to):
        t, a, b, _, _ = spans[c]
        for j in range(t, t + a + b):
            remote(
                code.at[to, :, pl.ds(j * LANES, LANES)], codes.at[:, lanes_of(j * NY + y)],
                s_o.at[c, 0], r_o.at[c, 0], **{AY: to},
            ).start()
        remote(scale.at[to, pl.ds(t, a + b)], scales.at[pl.ds(t, a + b), y], s_o.at[c, 1], r_o.at[c, 1], **{AY: to}).start()

    def encode(c, low, high):
        t, a, b, _, _ = spans[c]
        w = (a + b) * LANES
        factor = 2.0 / jnp.sum(cz[:, 0:1, 0:1], axis=0)

        def one(i, carry):
            to = lax.rem(y + i + 1, NY)
            v = prod[pl.ds(pl.multiple_of(to * rows, 16), rows), :w]
            m = jnp.max(jnp.abs(v), axis=0, keepdims=True)
            r = jnp.where(m > 0.0, 1.0 / jnp.where(m > 0.0, m, 1.0), 0.0)
            u = (jnp.sqrt(jnp.abs(v) * r) * TOP_CODE + 0.5).astype(jnp.int32)
            code[to, :, t * LANES:t * LANES + w] = jnp.where(v < 0.0, -u, u).astype(jnp.int16)
            m = m * factor
            for j in range(a + b):
                scale[to, t + j] = m[:, j * LANES:(j + 1) * LANES]

            @pl.when(i > 0)
            def _():
                send_out(c, lax.rem(y + i, NY))

            return carry

        lax.fori_loop(low, high, one, 0)
        if high == NY:
            for j in range(t, t + a + b):
                codes[:, lanes_of(j * NY + y)] = code[y, :, j * LANES:(j + 1) * LANES]
                scales[j, y] = scale[y, j]

    def lanes_of(tile):
        return pl.ds(pl.multiple_of(tile * LANES, LANES), LANES)

    def receive(c):
        k = (NY - 1) * (spans[c][1] + spans[c][2])
        to = wrap(y + 1, NY)
        whole = codes.at[:, pl.ds(0, k * LANES)]
        remote(whole, whole, s_o.at[c, 0], r_o.at[c, 0], **{AY: to}).wait()
        sizes = scales.at[pl.ds(0, k), 0]
        remote(sizes, sizes, s_o.at[c, 1], r_o.at[c, 1], **{AY: to}).wait()

    waited = False
    for kind, c, d in ORDER:
        if kind in ("l2", "l3") and not waited:
            left_wait1()
            waited = True
        if kind == "l1":
            left_step1()
        elif kind == "l2":
            for way in sorted({d, NZ - d}):
                left_step2(way)
        elif kind == "l3":
            for way in sorted({d, (NZ - d) % NZ}):
                if d:
                    left_copy2(way).wait()
                left_step3(way)
        elif kind == "mm":
            if d == 1:
                rings[c][1].finish()
                rings[c][3].finish()
                if c == 0:
                    left_wait3()
                    transpose_left()
                multiply(c)
            else:
                encode(c, *((0, NY // 2) if d == 2 else (NY // 2, NY)))
        else:
            k = ("px", "pz", "qz", "qx").index(kind)
            if d == 1 and k in (1, 3):
                rings[c][k - 1].finish()
            rings[c][k].run(d)
    for c in range(len(CHUNKS)):
        receive(c)


def exchange(acts, ids):
    n = len(CHUNKS)
    tiles = sum(a + b for a, b in CHUNKS)
    t_x, t_z = (sum(c[i] for c in CHUNKS) for i in (0, 1))
    slab = NY * NE * CAP
    wide = max(a + b for a, b in CHUNKS) * LANES
    rows = tiles * LANES // (NX * NZ)
    bf16, f32, i16 = jnp.bfloat16, jnp.float32, jnp.int16
    dma = pltpu.SemaphoreType.DMA
    vmem = pl.BlockSpec(memory_space=pltpu.VMEM)
    return pl.pallas_call(
        kernel,
        out_shape=(
            jax.ShapeDtypeStruct((rows, tiles * NY * LANES), i16),
            jax.ShapeDtypeStruct((tiles, NY, 1, LANES), f32),
        ),
        in_specs=[vmem, vmem],
        out_specs=(vmem, vmem),
        scratch_shapes=[
            pltpu.VMEM((NY * NE, CAP, (tiles + 1) * LANES), bf16),
            pltpu.VMEM((NE * CAP, tiles * NY * LANES), f32),
            pltpu.VMEM((NY * NE, CAP, (tiles + 1) * LANES), bf16),
            pltpu.VMEM((slab, tiles * LANES), bf16),
            pltpu.VMEM((NX * slab, tiles * LANES // NX), bf16),
            pltpu.VMEM((NY, NZ, NX * slab, LANES), bf16),
            pltpu.VMEM((NY * LANES, NZ * NX * slab), bf16),
            pltpu.VMEM((NZ, NX * slab, t_x * LANES), bf16),
            pltpu.VMEM((NZ, NX * slab, t_z * LANES), bf16),
            pltpu.VMEM((NY * rows, wide), f32),
            pltpu.VMEM((NY, rows, tiles * LANES), i16),
            pltpu.VMEM((NY, tiles, 1, LANES), f32),
            pltpu.VMEM((NX, 8, LANES), f32),
            pltpu.VMEM((NZ, 8, LANES), f32),
            dma(()), dma(()),
            dma((2,)), dma((2,)),
            dma(()), dma(()),
            dma((NZ,)), dma((NZ,)),
            dma((NY,)), dma((NY,)),
            dma((n,)), dma((n,)),
            dma((n,)), dma((n, NZ // 2)),
            dma((n,)), dma((n, NZ // 2)),
            dma((n,)), dma((n, NX // 2)),
            dma((max(DIRECT, 1),)), dma((max(DIRECT, 1),)),
            dma((n, 2)), dma((n, 2)),
        ],
        compiler_params=pltpu.CompilerParams(
            collective_id=0, has_side_effects=True, vmem_limit_bytes=48 * 1024 * 1024
        ),
        name="exchange",
    )(acts, ids)


def shards(activations, expert_ids):
    ff = activations.shape[1]
    codes, scales = exchange(activations, expert_ids)
    u = codes.astype(jnp.float32) * (1.0 / TOP_CODE)
    return (u * jnp.abs(u) * scales.reshape(1, ff))[None]


def solution(mesh):
    split = Mesh(mesh.devices.reshape(NX, NZ, NY, NE), TOK_EXP)
    return jax.shard_map(
        shards,
        mesh=split,
        in_specs=(P(TOK_EXP, None), P(TOK_EXP, None)),
        out_specs=P(AE, TOK, None),
        check_vma=False,
    )
```
